512 devices in a mesh: gx: 16 (over z_hi, y), gy: 32 (over z_lo, x, core).
Axes of the slice: x: 4, y: 4, z: 16 (z_hi: 4, z_lo: 4; z = z_hi * 4 + z_lo), core: 2. Of those that a mesh axis runs over, the one named last changes fastest.
Arguments:
- density: float32 [128, 512, 128], P('gx', 'gy'), may hold values from -3 to 3
- populations: float32 [19, 64, 64, 256], P(None, 'gx', 'gy'), may hold values from 0 to 0.6, as said below
Outputs:
- density_next: float32 [128, 512, 128], P('gx', 'gy')
- populations_next: float32 [19, 64, 64, 256], P(None, 'gx', 'gy')
The draws below stay inside these ranges and needn't reach their ends.
Inputs may be any that keep to these rules, and one draw needn't show every extreme that they name: `populations`: each population is its lattice weight times a factor between 0.4 and 1.6.
All inputs are finite; a program needn't handle non-finite values.
Results may differ from the reference program's by a relative error of at most 0.00023.
Values sent between devices are 32-bit elements; how exact they have to be, the bound alone decides.
A program may use at most 64 MiB of HBM per device.

```python
import jax
import jax.numpy as jnp
from jax import lax

NZ = 128
DENSITY_SUBSTEPS = 2
LATTICE_SPEEDS = 19
NX = 128
NY = 512
NXC = 64
NYC = 256
NZC = 64


def lattice_weights():
    return jnp.array([1.0 / 3.0] + [1.0 / 18.0] * 6 + [1.0 / 36.0] * 12, jnp.float32)


def draw_density(key, part):
    jagged = 0.7 * jax.random.truncated_normal(key, -4.0, 4.0, (NX, NY, NZ), jnp.float32)
    return jagged


def draw_populations(key, part):
    weights = lattice_weights()[:, None, None, None]
    factor = jax.random.uniform(key, (LATTICE_SPEEDS, NXC, NZC, NYC), jnp.float32, 0.6, 1.4)
    return weights * factor


def setup_inputs(seed: int = 0) -> dict:
    streams_of = jax.random.split(jax.random.key(seed), 3)
    density = draw_density(jax.random.fold_in(streams_of[2], 71), 0)
    populations = draw_populations(jax.random.fold_in(streams_of[2], 71), 0)
    return dict(density=density, populations=populations)


coupled_time_step = 8e-4
force_unit = 5e-3
speed_unit = 2000.0
relax_time = 0.8
quench_depth = -0.25


def lattice():
    speeds = [(0, 0, 0), (1, 0, 0), (-1, 0, 0), (0, 1, 0), (0, -1, 0), (0, 0, 1), (0, 0, -1),
              (1, 1, 0), (-1, -1, 0), (1, -1, 0), (-1, 1, 0), (1, 0, 1), (-1, 0, -1), (1, 0, -1),
              (-1, 0, 1), (0, 1, 1), (0, -1, -1), (0, 1, -1), (0, -1, 1)]
    weights = [1.0 / 3.0] + [1.0 / 18.0] * 6 + [1.0 / 36.0] * 12
    return speeds, weights


def laplace(grid_field):
    running = -6.0 * grid_field
    for dimension in range(3):
        running = running + jnp.roll(grid_field, 1, dimension) + jnp.roll(grid_field, -1, dimension)
    return running


def potential_of(grid_field):
    first_lap = laplace(grid_field)
    return quench_depth * grid_field + grid_field + 2.0 * first_lap + laplace(first_lap) + grid_field * grid_field * grid_field


def central(grid_field, dimension):
    return (jnp.roll(grid_field, -1, dimension) - jnp.roll(grid_field, 1, dimension)) * 0.5


def coarse_mean(grid_field):
    return grid_field.reshape(NX // 2, 2, NY // 2, 2, NZ // 2, 2).mean(axis=(1, 3, 5))


def reference(density, populations):
    speeds, weights = lattice()
    potential = potential_of(density)
    pieces = []
    for dimension in range(3):
        pieces.append(force_unit * coarse_mean(-density * central(potential, dimension)).transpose(0, 2, 1))
    coarse_force = jnp.stack(pieces)
    speed_table = jnp.array(speeds, jnp.float32)
    fluid_mass = jnp.sum(populations, axis=0)
    moment = jnp.einsum("qc,qxzy->cxzy", speed_table, populations, precision=lax.Precision.HIGHEST)
    flow_velocity = (moment + 0.5 * coarse_force) / fluid_mass
    speed_square = flow_velocity[0] * flow_velocity[0] + flow_velocity[1] * flow_velocity[1] + flow_velocity[2] * flow_velocity[2]
    force_velocity = flow_velocity[0] * coarse_force[0] + flow_velocity[1] * coarse_force[1] + flow_velocity[2] * coarse_force[2]
    source_gain = 1.0 - 0.5 / relax_time
    passed = []
    for member in range(LATTICE_SPEEDS):
        jump_x, jump_y, jump_z = speeds[member]
        lattice_weight = weights[member]
        projected = float(jump_x) * flow_velocity[0] + float(jump_y) * flow_velocity[1] + float(jump_z) * flow_velocity[2]
        force_along = float(jump_x) * coarse_force[0] + float(jump_y) * coarse_force[1] + float(jump_z) * coarse_force[2]
        balance = lattice_weight * fluid_mass * (1.0 + 3.0 * projected + 4.5 * projected * projected - 1.5 * speed_square)
        relaxed = populations[member] - (populations[member] - balance) / relax_time + source_gain * lattice_weight * (3.0 * (force_along - force_velocity) + 9.0 * projected * force_along)
        passed.append(jnp.roll(jnp.roll(jnp.roll(relaxed, jump_x, 0), jump_z, 1), jump_y, 2))
    populations_next = jnp.stack(passed)
    fine_velocity = (speed_unit * flow_velocity).transpose(0, 1, 3, 2)
    fine_velocity = jnp.repeat(jnp.repeat(jnp.repeat(fine_velocity, 2, 1), 2, 2), 2, 3)
    current = density
    for inner_substep in range(DENSITY_SUBSTEPS):
        if inner_substep > 0:
            potential = potential_of(current)
        advect = fine_velocity[0] * central(current, 0) + fine_velocity[1] * central(current, 1) + fine_velocity[2] * central(current, 2)
        current = current + coupled_time_step * (laplace(potential) - advect)
    return current, populations_next
```

```python
import jax
import jax.numpy as jnp
from jax import lax
from jax.experimental import pallas as pl
from jax.experimental.pallas import tpu as pltpu
from jax.sharding import PartitionSpec as P

MESH = pl.DeviceIdType.MESH
EXACT = lax.Precision.HIGHEST
F32 = jnp.float32

TIME_STEP = 0.0008
FORCE_UNIT = 0.005
SPEED_UNIT = 2000.0
RELAX_TIME = 0.8
QUENCH = -0.25

SPEEDS = [
    (0, 0, 0),
    (1, 0, 0), (-1, 0, 0), (0, 1, 0), (0, -1, 0), (0, 0, 1), (0, 0, -1),
    (1, 1, 0), (-1, -1, 0), (1, -1, 0), (-1, 1, 0),
    (1, 0, 1), (-1, 0, -1), (1, 0, -1), (-1, 0, 1),
    (0, 1, 1), (0, -1, -1), (0, 1, -1), (0, -1, 1),
]
WEIGHTS = [1.0 / 3.0] + [1.0 / 18.0] * 6 + [1.0 / 36.0] * 12

ORDER = [13, 1, 7, 9, 11, 5, 15, 18, 14, 2, 8, 10, 12, 6, 16, 17, 13, 0, 3, 4]
RISE_X, RISE_Z, FALL_X, FALL_Z = 0, 4, 8, 12
SLOT = {}
for _place, _member in enumerate(ORDER):
    SLOT.setdefault(_member, _place)
MASS = 20
FIELDS = 24


def dot_t(a, b):
    return lax.dot_general(
        a, b, (((1,), (1,)), ((), ())), precision=EXACT, preferred_element_type=F32
    )


def t_dot(a, b):
    return lax.dot_general(
        a, b, (((0,), (0,)), ((), ())), precision=EXACT, preferred_element_type=F32
    )


def iota(shape, dim):
    return lax.broadcasted_iota(jnp.int32, shape, dim)


def kernel(
    nx, n, dens_hbm, pops_hbm, dens_out, pops_out,
    E, E1, L1, PT, FA, FB, SP, SF, RF, SM, RM, MQ, NB, PV, EP, XS, XR, ZS, ZR, FR, RS, OP, OD,
    dsem, psem, odsem, opsem, xs_s, xs_r, ys_s, ys_r, cs_s, cs_r, x2_s, x2_r, y2_s, y2_r,
    c2_s, c2_r, px_s, px_r, pz_s, pz_r, ms_s, ms_r, fs_s, fs_r,
):
    L = 4 * n
    gx = lax.axis_index("gx")
    gy = lax.axis_index("gy")
    xu, xd = lax.rem(gx + 1, nx), lax.rem(gx + nx - 1, nx)
    yu, yd = lax.rem(gy + 1, n), lax.rem(gy + n - 1, n)
    UPX, DNX = {"gx": xu, "gy": gy}, {"gx": xd, "gy": gy}
    UPY, DNY = {"gx": gx, "gy": yu}, {"gx": gx, "gy": yd}

    barrier = pltpu.get_barrier_semaphore()
    for where in (UPX, DNX):
        pl.semaphore_signal(barrier, inc=1, device_id=where, device_id_type=MESH)

    @pl.loop(1, n)
    def _(k):
        pl.semaphore_signal(
            barrier, inc=1, device_id={"gx": gx, "gy": lax.rem(gy + k, n)}, device_id_type=MESH
        )

    dens_in = pltpu.make_async_copy(dens_hbm, E.at[pl.ds(5, 8), pl.ds(8, 16)], dsem)
    dens_in.start()
    pops_in = pltpu.make_async_copy(pops_hbm, PV, psem)
    pops_in.start()

    def remote(src, dst, send, recv, where):
        return pltpu.make_async_remote_copy(
            src_ref=src, dst_ref=dst, send_sem=send, recv_sem=recv, device_id=where,
            device_id_type=MESH,
        )

    lane = iota((1, L), 1)

    pops_in.wait()
    for h in range(2):
        for place, member in enumerate(ORDER):
            for x in range(4):
                EP[h, place, pl.ds(x * 4 + 5, 2), :] = PV[member, x, :, pl.ds(h * L, L)]
        total = jnp.zeros((24, L), F32)
        moment = [jnp.zeros((24, L), F32) for _ in range(3)]
        for member in range(19):
            value = EP[h, SLOT[member]]
            total = total + value
            for c in range(3):
                if SPEEDS[member][c] == 1:
                    moment[c] = moment[c] + value
                elif SPEEDS[member][c] == -1:
                    moment[c] = moment[c] - value
        EP[h, MASS] = total
        for c in range(3):
            EP[h, MASS + 1 + c] = moment[c]

    for way, (first, row) in enumerate(((RISE_X, 17), (FALL_X, 5))):
        for f in range(9):
            place = first + f if f < 5 else MASS + f - 5
            for h in range(2):
                XS[way, f * 2 + h] = EP[h, place, pl.ds(row, 2), :]

    spread = [
        (iota((n, L), 1) + h * L) // 8 == iota((n, L), 0) for h in range(2)
    ]
    spread = [jnp.where(s, 1.0, 0.0).astype(F32) for s in spread]
    for zl in range(2):
        result = None
        for h in range(2):
            for c in range(4):
                NB[h, pl.ds(c * 4, 4), :] = EP[h, MASS + c, pl.ds(5 + zl, 4, stride=4), :]
            block = NB[h]
            tiles = jnp.concatenate(
                [jnp.where(lax.rem(lane, 8) == y, block, 0.0) for y in range(8)], axis=0
            )
            part = dot_t(spread[h], tiles)
            result = part if result is None else result + part
        SM[pl.ds(zl, n, stride=8), :] = result

    dens_in.wait()
    pl.semaphore_wait(barrier, n + 1)

    def x_pair(buf, width, size, send, recv):
        lo = width
        return [
            remote(buf.at[pl.ds(lo + 8 - size, size), pl.ds(8, 16)],
                   buf.at[pl.ds(lo - size, size), pl.ds(8, 16)], send.at[0], recv.at[0], UPX),
            remote(buf.at[pl.ds(lo, size), pl.ds(8, 16)],
                   buf.at[pl.ds(lo + 8, size), pl.ds(8, 16)], send.at[1], recv.at[1], DNX),
        ]

    def y_pair(buf, x0, size, send, recv, k):
        return [
            remote(buf.at[pl.ds(x0, size), pl.ds(21, 3)],
                   buf.at[pl.ds(x0, size), pl.ds(5, 3)], send.at[k], recv.at[k], UPY),
            remote(buf.at[pl.ds(x0, size), pl.ds(8, 3)],
                   buf.at[pl.ds(x0, size), pl.ds(24, 3)], send.at[k + 1], recv.at[k + 1], DNY),
        ]

    halo_x = x_pair(E, 5, 5, xs_s, xs_r)
    halo_y = y_pair(E, 5, 8, ys_s, ys_r, 0)
    for copy in halo_x + halo_y:
        copy.start()

    def moment_copy(to, sem_to, slot):
        return remote(
            SM.at[pl.ds(pl.multiple_of(to * 8, 8), 2)],
            RM.at[pl.ds(pl.multiple_of(slot * 8, 8), 2)],
            ms_s.at[sem_to], ms_r.at[slot], {"gx": gx, "gy": to},
        )

    def force_copy(to, sem_to, slot):
        return remote(
            SF.at[pl.ds(pl.multiple_of(to * 8, 8), 5)],
            RF.at[pl.ds(pl.multiple_of(slot * 8, 8), 5)],
            fs_s.at[sem_to], fs_r.at[slot], {"gx": gx, "gy": to},
        )

    @pl.loop(1, n)
    def _(k):
        to = lax.rem(gy + k, n)
        moment_copy(to, to, gy).start()

    face_x = [
        remote(XS.at[0], XR.at[0], px_s.at[0], px_r.at[0], UPX),
        remote(XS.at[1], XR.at[1], px_s.at[1], px_r.at[1], DNX),
    ]
    for copy in face_x:
        copy.start()

    corners = []
    for way in range(2):
        halo_x[way].wait_recv()
        for copy in y_pair(E, 1 if way == 0 else 13, 4, cs_s, cs_r, 2 * way):
            copy.start()
            corners.append(copy)

    for way in range(2):
        face_x[way].wait_recv()
        first, row = ((RISE_X, 1), (FALL_X, 21))[way]
        for f in range(9):
            place = first + f if f < 5 else MASS + f - 5
            for h in range(2):
                EP[h, place, pl.ds(row, 2), :] = XR[way, f * 2 + h]
                if place == 0:
                    EP[h, 16, pl.ds(row, 2), :] = XR[way, f * 2 + h]
    for way, (first, zi) in enumerate(((RISE_Z, 2), (FALL_Z, 1))):
        for f in range(9):
            place = first + f if f < 5 else MASS + f - 5
            for h in range(2):
                ZS[way, h * 9 + f, pl.ds(0, 6), :] = EP[h, place, pl.ds(zi, 6, stride=4), :]
    face_z = [
        remote(ZS.at[0, :, pl.ds(0, 6)], ZR.at[0, :, pl.ds(0, 6)], pz_s.at[0], pz_r.at[0], UPY),
        remote(ZS.at[1, :, pl.ds(0, 6)], ZR.at[1, :, pl.ds(0, 6)], pz_s.at[1], pz_r.at[1], DNY),
    ]
    for copy in face_z:
        copy.start()

    own = pl.ds(pl.multiple_of(gy * 8, 8), 8)
    RM[own, :] = SM[own, :]

    @pl.loop(1, n)
    def _(k):
        frm = lax.rem(gy + k, n)
        moment_copy(frm, frm, frm).wait_recv()

    both = jnp.concatenate([RM[pl.ds(zl, n, stride=8), :] for zl in range(2)], axis=0)
    shape = (2 * n, L)
    row = iota(shape, 0)
    pick = iota(shape, 1) // 2 == 2 * lax.rem(row, n) + row // n
    wide = t_dot(both, jnp.where(pick, 1.0, 0.0).astype(F32))
    for y in range(8):
        MQ[pl.ds(y * 32, 16), :] = wide[y * 16:(y + 1) * 16]
        MQ[pl.ds(y * 32 + 16, 16), :] = wide[y * 16:(y + 1) * 16]

    for copy in halo_y + corners:
        copy.wait_recv()

    def turn(value, by):
        return pltpu.roll(value, by % L, 1)

    def lap(ref, i, r0, rows):
        c = ref[i, pl.ds(r0, rows), :]
        return c, (
            -6.0 * c + ref[i - 1, pl.ds(r0, rows), :] + ref[i + 1, pl.ds(r0, rows), :]
            + ref[i, pl.ds(r0 - 1, rows), :] + ref[i, pl.ds(r0 + 1, rows), :]
            + turn(c, 1) + turn(c, -1)
        )

    def potential(src, layers):
        @pl.loop(0, layers + 2)
        def _(i):
            L1[i, pl.ds(0, 24), :] = lap(src, i + 1, 6, 24)[1]

        @pl.loop(0, layers)
        def _(j):
            c, second = lap(L1, j + 1, 1, 24)
            rho = src[j + 2, pl.ds(7, 24), :]
            PT[j, pl.ds(0, 24), :] = (
                (QUENCH + 1.0) * rho + 2.0 * c + second + rho * rho * rho
            )

    potential(E, 14)

    scale = -0.5 * FORCE_UNIT * 0.125
    zeros = jnp.zeros((16, L), F32)
    for extra in range(8, 16):
        FB[pl.ds(extra, 16, stride=16), :] = zeros
    for xi in range(6):
        sums = [None, None, None]
        for k in (2 * xi, 2 * xi + 1):
            rho = E[k + 3, pl.ds(8, 16), :] * scale
            mid = PT[k + 1, pl.ds(1, 16), :]
            parts = (
                PT[k + 2, pl.ds(1, 16), :] - PT[k, pl.ds(1, 16), :],
                PT[k + 1, pl.ds(2, 16), :] - PT[k + 1, pl.ds(0, 16), :],
                turn(mid, -1) - turn(mid, 1),
            )
            for c in range(3):
                value = rho * parts[c]
                sums[c] = value if sums[c] is None else sums[c] + value
        for c in range(3):
            cx = c * 6 + xi
            if 1 <= xi <= 4:
                SP[c * 4 + xi - 1] = sums[c]
            if cx < 16:
                FA[pl.ds(cx, 16, stride=16), :] = sums[c]
            else:
                for zl in range(4):
                    FB[pl.ds((cx - 16) * 4 + zl, 16, stride=16), :] = turn(
                        sums[c], -2 * (zl - 1)
                    )
    shape = (4 * n, L)
    row = iota(shape, 0)
    window = lax.rem(2 * lax.rem(row, n) - 1 + row // n + 2 * n, 2 * n)
    choose = jnp.where(iota(shape, 1) // 2 == window, 1.0, 0.0).astype(F32)
    ga = jnp.concatenate(
        [FA[pl.ds(32 * y, 16), :] + FA[pl.ds(32 * y + 16, 16), :] for y in range(8)], axis=0
    )
    gb = jnp.concatenate(
        [FB[pl.ds(32 * y, 16), :] + FB[pl.ds(32 * y + 16, 16), :] for y in range(8)], axis=0
    )
    ta = dot_t(choose, ga)
    tb = dot_t(choose[n:2 * n], gb)
    for zl in range(4):
        SF[pl.ds(zl, n, stride=8), :] = ta[zl * n:(zl + 1) * n]
    SF[pl.ds(4, n, stride=8), :] = tb

    @pl.loop(1, n)
    def _(k):
        to = lax.rem(gy + k, n)
        force_copy(to, to, gy).start()

    for slot in range(5):
        RF[pl.ds(gy * 8 + slot, 1), :] = SF[pl.ds(gy * 8 + slot, 1), :]

    even_y = lax.rem(iota((16, L), 0), 2) == 0
    even_z = lax.rem(iota((16, L), 1), 2) == 0

    def fine_speed(x):
        mass = MQ[pl.ds(x, 16, stride=16), :]
        inverse = SPEED_UNIT * 0.5 / mass
        out = []
        for c in range(3):
            s = SP[c * 4 + x]
            s = s + jnp.where(even_y, pltpu.roll(s, 15, 0), pltpu.roll(s, 1, 0))
            s = s + jnp.where(even_z, turn(s, -1), turn(s, 1))
            m = MQ[pl.ds((c + 1) * 4 + x, 16, stride=16), :]
            out.append((m + 0.5 * s) * inverse)
        return out

    def advance(src, e, p, speed):
        mid = src[e, pl.ds(8, 16), :]
        advect = (
            speed[0] * (src[e + 1, pl.ds(8, 16), :] - src[e - 1, pl.ds(8, 16), :])
            + speed[1] * (src[e, pl.ds(9, 16), :] - src[e, pl.ds(7, 16), :])
            + speed[2] * (turn(mid, -1) - turn(mid, 1))
        )
        return mid + TIME_STEP * (lap(PT, p, 1, 16)[1] - advect)

    for x in range(4):
        speed = fine_speed(x)
        for c in range(3):
            SP[c * 4 + x] = speed[c]
        for k in (2 * x, 2 * x + 1):
            E1[k + 3, pl.ds(8, 16), :] = advance(E, k + 5, k + 3, speed)

    again_x = x_pair(E1, 3, 3, x2_s, x2_r)
    again_y = y_pair(E1, 3, 8, y2_s, y2_r, 0)
    for copy in again_x + again_y:
        copy.start()

    for way in range(2):
        face_z[way].wait_recv()
        first, zi = ((RISE_Z, 0), (FALL_Z, 3))[way]
        for f in range(9):
            place = first + f if f < 5 else MASS + f - 5
            if place == 16:
                place = 0
            for h in range(2):
                EP[h, place, pl.ds(zi, 6, stride=4), :] = ZR[way, h * 9 + f, pl.ds(0, 6), :]

    corners2 = []
    for way in range(2):
        again_x[way].wait_recv()
        for copy in y_pair(E1, 1 if way == 0 else 11, 2, c2_s, c2_r, 2 * way):
            copy.start()
            corners2.append(copy)

    @pl.loop(1, n)
    def _(k):
        frm = lax.rem(gy + k, n)
        force_copy(frm, frm, frm).wait_recv()

    half = n // 2
    expand = jnp.where(iota((half, L), 1) // 8 == iota((half, L), 0), 1.0, 0.0).astype(F32)
    for slot in range(5):
        whole = RF[pl.ds(slot, n, stride=8), :]
        for h in range(2):
            q = t_dot(whole[h * half:(h + 1) * half], expand)
            value = q[0:16]
            for y in range(1, 8):
                value = jnp.where(lax.rem(lane, 8) == y, q[y * 16:(y + 1) * 16], value)
            if slot < 4:
                FR[h, pl.ds(slot, 16, stride=4), :] = value
            else:
                FR[h, pl.ds(64, 16), :] = value

    state = []
    for h in range(2):
        mass = EP[h, MASS]
        inverse = 1.0 / mass
        force = [FR[h, pl.ds(c * 24, 24), :] for c in range(3)]
        flow = [(EP[h, MASS + 1 + c] + 0.5 * force[c]) * inverse for c in range(3)]
        square = flow[0] * flow[0] + flow[1] * flow[1] + flow[2] * flow[2]
        work = flow[0] * force[0] + flow[1] * force[1] + flow[2] * force[2]
        state.append((mass, force, flow, 1.0 - 1.5 * square, work))
    rate = 1.0 / RELAX_TIME
    gain = 1.0 - 0.5 / RELAX_TIME

    def along(speed, vector):
        out = None
        for c in range(3):
            if speed[c] == 1:
                out = vector[c] if out is None else out + vector[c]
            elif speed[c] == -1:
                out = -vector[c] if out is None else out - vector[c]
        return out

    for member in range(19):
        cx, cy, cz = SPEEDS[member]
        w = WEIGHTS[member]
        parts = []
        for h in range(2):
            mass, force, flow, rest, work = state[h]
            p = EP[h, SLOT[member]]
            if member == 0:
                new = (rate * w) * mass * rest - (3.0 * gain * w) * work
            else:
                cu, cf = along(SPEEDS[member], flow), along(SPEEDS[member], force)
                new = (rate * w) * mass * (rest + cu * (3.0 + 4.5 * cu)) + (gain * w) * (
                    3.0 * (cf - work) + 9.0 * cu * cf
                )
            parts.append(p * (1.0 - rate) + new)
        if cy:
            turned = [pltpu.roll(v, cy % L, 1) for v in parts]
            edge = lane == (0 if cy == 1 else L - 1)
            parts = [jnp.where(edge, turned[1 - h], turned[h]) for h in range(2)]
        for h in range(2):
            RS[member, h] = parts[h]
            for x in range(4):
                OP[member, x, :, pl.ds(h * L, L)] = RS[
                    member, h, pl.ds((x + 1 - cx) * 4 + 1 - cz, 2), :
                ]
    pops_end = pltpu.make_async_copy(OP, pops_out, opsem)
    pops_end.start()

    for copy in again_y + corners2:
        copy.wait_recv()
    potential(E1, 10)
    for x in range(4):
        speed = [SP[c * 4 + x] for c in range(3)]
        for k in (2 * x, 2 * x + 1):
            OD[k] = advance(E1, k + 3, k + 1, speed)
    dens_end = pltpu.make_async_copy(OD, dens_out, odsem)
    dens_end.start()

    for copy in halo_x + halo_y + corners + face_x + face_z + again_x + again_y + corners2:
        copy.wait_send()

    @pl.loop(1, n)
    def _(k):
        to = lax.rem(gy + k, n)
        moment_copy(to, to, gy).wait_send()
        force_copy(to, to, gy).wait_send()

    pops_end.wait()
    dens_end.wait()


def solution(mesh):
    nx, n = mesh.shape["gx"], mesh.shape["gy"]
    L = 4 * n

    def local(density, populations):
        vmem = lambda *shape: pltpu.VMEM(shape, F32)
        dma = lambda *shape: pltpu.SemaphoreType.DMA(shape)
        any_spec = pl.BlockSpec(memory_space=pl.ANY)
        return pl.pallas_call(
            lambda *refs: kernel(nx, n, *refs),
            out_shape=(
                jax.ShapeDtypeStruct((8, 16, L), F32),
                jax.ShapeDtypeStruct((19, 4, 2, 2 * L), F32),
            ),
            in_specs=[any_spec, any_spec],
            out_specs=(any_spec, any_spec),
            scratch_shapes=[
                vmem(18, 32, L), vmem(14, 32, L), vmem(16, 32, L), vmem(14, 32, L),
                vmem(256, L), vmem(256, L), vmem(12, 16, L),
                vmem(n * 8, 128), vmem(n * 8, 128), vmem(n * 8, 128), vmem(n * 8, 128),
                vmem(256, L), vmem(2, 16, L), vmem(19, 4, 2, 2 * L),
                vmem(2, FIELDS, 24, L), vmem(2, 18, 2, L), vmem(2, 18, 2, L),
                vmem(2, 18, 8, L), vmem(2, 18, 8, L), vmem(2, 80, L),
                vmem(19, 2, 24, L), vmem(19, 4, 2, 2 * L), vmem(8, 16, L),
                pltpu.SemaphoreType.DMA, pltpu.SemaphoreType.DMA,
                pltpu.SemaphoreType.DMA, pltpu.SemaphoreType.DMA,
                dma(2), dma(2), dma(2), dma(2), dma(4), dma(4),
                dma(2), dma(2), dma(2), dma(2), dma(4), dma(4),
                dma(2), dma(2), dma(2), dma(2),
                dma(n), dma(n), dma(n), dma(n),
            ],
            compiler_params=pltpu.CompilerParams(collective_id=0, has_side_effects=True),
        )(density, populations)

    return jax.shard_map(
        local,
        mesh=mesh,
        in_specs=(P("gx", "gy", None), P(None, "gx", "gy", None)),
        out_specs=(P("gx", "gy", None), P(None, "gx", "gy", None)),
        check_vma=False,
    )
```

```python
import jax
import jax.numpy as jnp
from jax import lax
from jax.experimental import pallas as pl
from jax.experimental.pallas import tpu as pltpu
from jax.sharding import PartitionSpec as P

MESH = pl.DeviceIdType.MESH
EXACT = lax.Precision.HIGHEST
F32 = jnp.float32

TIME_STEP = 0.0008
FORCE_UNIT = 0.005
SPEED_UNIT = 2000.0
RELAX_TIME = 0.8
QUENCH = -0.25

SPEEDS = [
    (0, 0, 0),
    (1, 0, 0), (-1, 0, 0), (0, 1, 0), (0, -1, 0), (0, 0, 1), (0, 0, -1),
    (1, 1, 0), (-1, -1, 0), (1, -1, 0), (-1, 1, 0),
    (1, 0, 1), (-1, 0, -1), (1, 0, -1), (-1, 0, 1),
    (0, 1, 1), (0, -1, -1), (0, 1, -1), (0, -1, 1),
]
WEIGHTS = [1.0 / 3.0] + [1.0 / 18.0] * 6 + [1.0 / 36.0] * 12

MASS = 19
FIELDS = 23
RISE_X = [q for q in range(19) if SPEEDS[q][0] == 1]
FALL_X = [q for q in range(19) if SPEEDS[q][0] == -1]
RISE_Z = [q for q in range(19) if SPEEDS[q][2] == 1]
FALL_Z = [q for q in range(19) if SPEEDS[q][2] == -1]
MOMENTS = [MASS, MASS + 1, MASS + 2, MASS + 3]
DIAGONALS = [(1, 1), (1, -1), (-1, 1), (-1, -1)]


def dot_t(a, b):
    return lax.dot_general(
        a, b, (((1,), (1,)), ((), ())), precision=EXACT, preferred_element_type=F32
    )


def t_dot(a, b):
    return lax.dot_general(
        a, b, (((0,), (0,)), ((), ())), precision=EXACT, preferred_element_type=F32
    )


def iota(shape, dim):
    return lax.broadcasted_iota(jnp.int32, shape, dim)


def kernel(
    nx, n, dens_hbm, pops_hbm, OD, OP,
    E, E1, L1, PT, FA, FB, SP, SF, RF, SM, RM, MQ, MX, PV, EP, XS, XR, ZS, ZR, DS, DR, FR, RS,
    dsem, psem, dx_s, dx_r, dy_s, dy_r, dd_s, dd_r, px_s, px_r, pz_s, pz_r, pd_s, pd_r,
    ms_s, ms_r, fs_s, fs_r,
):
    L = 4 * n
    gx = lax.axis_index("gx")
    gy = lax.axis_index("gy")

    def place(sx, sy):
        return {"gx": lax.rem(gx + sx + nx, nx), "gy": lax.rem(gy + sy + n, n)}

    barrier = pltpu.get_barrier_semaphore()
    for sx, sy in DIAGONALS + [(1, 0), (-1, 0)]:
        pl.semaphore_signal(barrier, inc=1, device_id=place(sx, sy), device_id_type=MESH)

    @pl.loop(1, n)
    def _(k):
        pl.semaphore_signal(barrier, inc=1, device_id=place(0, k), device_id_type=MESH)

    dens_in = pltpu.make_async_copy(dens_hbm, E.at[pl.ds(7, 8), pl.ds(8, 16)], dsem)
    dens_in.start()
    pops_in = pltpu.make_async_copy(pops_hbm, PV, psem)
    pops_in.start()

    def remote(src, dst, send, recv, where):
        return pltpu.make_async_remote_copy(
            src_ref=src, dst_ref=dst, send_sem=send, recv_sem=recv, device_id=where,
            device_id_type=MESH,
        )

    def block(x0, xs, y0, ys):
        return E.at[pl.ds(x0, xs), pl.ds(y0, ys)]

    dens_in.wait()
    pl.semaphore_wait(barrier, n + 5)

    halo = []
    for i, (sx, sy) in enumerate(DIAGONALS):
        x0, x1 = (9, 1) if sx == 1 else (7, 15)
        y0, y1 = (18, 2) if sy == 1 else (8, 24)
        halo.append(remote(
            block(x0, 6, y0, 6), block(x1, 6, y1, 6), dd_s.at[i], dd_r.at[i], place(sx, sy)
        ))
    halo += [
        remote(block(8, 7, 8, 16), block(0, 7, 8, 16), dx_s.at[0], dx_r.at[0], place(1, 0)),
        remote(block(7, 7, 8, 16), block(15, 7, 8, 16), dx_s.at[1], dx_r.at[1], place(-1, 0)),
        remote(block(7, 8, 17, 7), block(7, 8, 1, 7), dy_s.at[0], dy_r.at[0], place(0, 1)),
        remote(block(7, 8, 8, 7), block(7, 8, 24, 7), dy_s.at[1], dy_r.at[1], place(0, -1)),
    ]
    for copy in halo:
        copy.start()

    lane = iota((1, L), 1)

    pops_in.wait()
    for h in range(2):
        for member in range(19):
            for x in range(4):
                EP[h, member, pl.ds(x * 4 + 5, 2), :] = PV[member, x, :, pl.ds(h * L, L)]
        total = jnp.zeros((24, L), F32)
        moment = [jnp.zeros((24, L), F32) for _ in range(3)]
        for member in range(19):
            value = EP[h, member]
            total = total + value
            for c in range(3):
                if SPEEDS[member][c] == 1:
                    moment[c] = moment[c] + value
                elif SPEEDS[member][c] == -1:
                    moment[c] = moment[c] - value
        EP[h, MASS] = total
        for c in range(3):
            EP[h, MASS + 1 + c] = moment[c]

    for way, (members, row, rows) in enumerate(
        ((RISE_X, 17, (13, 17)), (FALL_X, 5, (5, 9)))
    ):
        for h in range(2):
            for f in range(5):
                XS[way, f * 2 + h] = EP[h, members[f], pl.ds(row, 2), :]
            for c in range(4):
                for layer in range(2):
                    XS[way, 10 + (c * 2 + layer) * 2 + h] = EP[
                        h, MASS + c, pl.ds(rows[layer], 2), :
                    ]
    face_x = [
        remote(XS.at[0], XR.at[0], px_s.at[0], px_r.at[0], place(1, 0)),
        remote(XS.at[1], XR.at[1], px_s.at[1], px_r.at[1], place(-1, 0)),
    ]
    for copy in face_x:
        copy.start()

    for way, (members, zi) in enumerate(((RISE_Z, 2), (FALL_Z, 1))):
        for f, field in enumerate(members + MOMENTS):
            for h in range(2):
                ZS[way, f * 2 + h] = EP[h, field, pl.ds(4 + zi, 4, stride=4), :]
    for i, (sx, sy) in enumerate(DIAGONALS):
        row = (16 if sx == 1 else 4) + (2 if sy == 1 else 1)
        for f, field in enumerate([SPEEDS.index((sx, 0, sy))] + MOMENTS):
            for h in range(2):
                DS[i, pl.ds(f * 2 + h, 1), :] = EP[h, field, pl.ds(row, 1), :]
    face_z = [
        remote(ZS.at[0], ZR.at[0], pz_s.at[0], pz_r.at[0], place(0, 1)),
        remote(ZS.at[1], ZR.at[1], pz_s.at[1], pz_r.at[1], place(0, -1)),
    ]
    edges = [
        remote(DS.at[i], DR.at[i], pd_s.at[i], pd_r.at[i], place(sx, sy))
        for i, (sx, sy) in enumerate(DIAGONALS)
    ]
    for copy in edges + face_z:
        copy.start()

    for h in range(2):
        for zl in range(2):
            for c in range(4):
                MX[zl, h, pl.ds(c * 8 + 2, 4), :] = EP[h, MASS + c, pl.ds(5 + zl, 4, stride=4), :]
    for way in range(2):
        face_x[way].wait_recv()
        for h in range(2):
            for c in range(4):
                for layer in range(2):
                    both = XR[way, 10 + (c * 2 + layer) * 2 + h]
                    for zl in range(2):
                        MX[zl, h, pl.ds(c * 8 + way * 6 + layer, 1), :] = both[zl:zl + 1]
    shape = (3 * n, L)
    row, col = iota(shape, 0), iota(shape, 1)
    spread = []
    for h in range(2):
        t = lax.rem(col + (h * L + 2 + 8 * n) - 4 * (row // n), 8 * n)
        hit = jnp.logical_and(t // 8 == lax.rem(row, n), lax.rem(t, 8) < 4)
        spread.append(jnp.where(hit, 1.0, 0.0).astype(F32))
    for zl in range(2):
        result = None
        for h in range(2):
            values = MX[zl, h]
            tiles = jnp.concatenate(
                [jnp.where(lax.rem(lane + 2, 4) == y, values, 0.0) for y in range(4)], axis=0
            )
            part = dot_t(spread[h], tiles)
            result = part if result is None else result + part
        for yg in range(3):
            SM[pl.ds(zl * 3 + yg, n, stride=8), :] = result[yg * n:(yg + 1) * n]

    def moment_copy(to, sem_to, slot):
        return remote(
            SM.at[pl.ds(pl.multiple_of(to * 8, 8), 6)],
            RM.at[pl.ds(pl.multiple_of(slot * 8, 8), 6)],
            ms_s.at[sem_to], ms_r.at[slot], {"gx": gx, "gy": to},
        )

    def force_copy(to, sem_to, slot):
        return remote(
            SF.at[pl.ds(pl.multiple_of(to * 8, 8), 5)],
            RF.at[pl.ds(pl.multiple_of(slot * 8, 8), 5)],
            fs_s.at[sem_to], fs_r.at[slot], {"gx": gx, "gy": to},
        )

    @pl.loop(1, n)
    def _(k):
        to = lax.rem(gy + k, n)
        moment_copy(to, to, gy).start()

    for slot in range(6):
        RM[pl.ds(gy * 8 + slot, 1), :] = SM[pl.ds(gy * 8 + slot, 1), :]

    for way, (members, row, layer) in enumerate(((RISE_X, 1, 1), (FALL_X, 21, 0))):
        for h in range(2):
            for f in range(5):
                EP[h, members[f], pl.ds(row, 2), :] = XR[way, f * 2 + h]
            for c in range(4):
                EP[h, MASS + c, pl.ds(row, 2), :] = XR[way, 10 + (c * 2 + layer) * 2 + h]

    def turn(value, by):
        return pltpu.roll(value, by % L, 1)

    def lap(ref, i, r0, rows):
        c = ref[i, pl.ds(r0, rows), :]
        return c, (
            -6.0 * c + ref[i - 1, pl.ds(r0, rows), :] + ref[i + 1, pl.ds(r0, rows), :]
            + ref[i, pl.ds(r0 - 1, rows), :] + ref[i, pl.ds(r0 + 1, rows), :]
            + turn(c, 1) + turn(c, -1)
        )

    def potential(src, layers, r0, rows):
        @pl.loop(0, layers + 2)
        def _(i):
            L1[i, pl.ds(0, rows), :] = lap(src, i + 1, r0, rows)[1]

        @pl.loop(0, layers)
        def _(j):
            c, second = lap(L1, j + 1, 1, rows)
            rho = src[j + 2, pl.ds(r0 + 1, rows), :]
            PT[j, pl.ds(0, rows), :] = (
                (QUENCH + 1.0) * rho + 2.0 * c + second + rho * rho * rho
            )

    for copy in halo:
        copy.wait_recv()
    potential(E, 18, 2, 32)

    scale = -0.5 * FORCE_UNIT * 0.125
    zeros = jnp.zeros((16, L), F32)
    for extra in range(8, 16):
        FB[pl.ds(extra, 16, stride=16), :] = zeros

    def force_pair(x8):
        sums = [None, None, None]
        for k in (2 * x8, 2 * x8 + 1):
            rho = E[k + 3, pl.ds(4, 24), :] * scale
            mid = PT[k + 1, pl.ds(1, 24), :]
            parts = (
                PT[k + 2, pl.ds(1, 24), :] - PT[k, pl.ds(1, 24), :],
                PT[k + 1, pl.ds(2, 24), :] - PT[k + 1, pl.ds(0, 24), :],
                turn(mid, -1) - turn(mid, 1),
            )
            for c in range(3):
                value = rho * parts[c]
                sums[c] = value if sums[c] is None else sums[c] + value
        for c in range(3):
            SP[c * 8 + x8] = sums[c]

    for x8 in range(1, 7):
        force_pair(x8)
        for c in range(3):
            cx = c * 6 + x8 - 1
            own = SP[c * 8 + x8, pl.ds(4, 16), :]
            if cx < 16:
                FA[pl.ds(cx, 16, stride=16), :] = own
            else:
                for zl in range(4):
                    FB[pl.ds((cx - 16) * 4 + zl, 16, stride=16), :] = turn(own, -2 * (zl - 1))
    shape = (4 * n, L)
    row = iota(shape, 0)
    window = lax.rem(2 * lax.rem(row, n) - 1 + row // n + 2 * n, 2 * n)
    choose = jnp.where(iota(shape, 1) // 2 == window, 1.0, 0.0).astype(F32)
    ga = jnp.concatenate(
        [FA[pl.ds(32 * y, 16), :] + FA[pl.ds(32 * y + 16, 16), :] for y in range(8)], axis=0
    )
    gb = jnp.concatenate(
        [FB[pl.ds(32 * y, 16), :] + FB[pl.ds(32 * y + 16, 16), :] for y in range(8)], axis=0
    )
    ta = dot_t(choose, ga)
    tb = dot_t(choose[n:2 * n], gb)
    for zl in range(4):
        SF[pl.ds(zl, n, stride=8), :] = ta[zl * n:(zl + 1) * n]
    SF[pl.ds(4, n, stride=8), :] = tb

    @pl.loop(1, n)
    def _(k):
        to = lax.rem(gy + k, n)
        force_copy(to, to, gy).start()

    for slot in range(5):
        RF[pl.ds(gy * 8 + slot, 1), :] = SF[pl.ds(gy * 8 + slot, 1), :]
    force_pair(0)
    force_pair(7)

    for way, (members, zi) in enumerate(((RISE_Z, 0), (FALL_Z, 3))):
        face_z[way].wait_recv()
        for f, field in enumerate(members + MOMENTS):
            for h in range(2):
                EP[h, field, pl.ds(4 + zi, 4, stride=4), :] = ZR[way, f * 2 + h]
    for i, (sx, sy) in enumerate(DIAGONALS):
        edges[i].wait_recv()
        row = (0 if sx == 1 else 20) + (0 if sy == 1 else 3)
        for f, field in enumerate([SPEEDS.index((sx, 0, sy))] + MOMENTS):
            for h in range(2):
                EP[h, field, pl.ds(row, 1), :] = DR[i, pl.ds(f * 2 + h, 1), :]

    @pl.loop(1, n)
    def _(k):
        frm = lax.rem(gy + k, n)
        moment_copy(frm, frm, frm).wait_recv()

    shape = (2 * n, L)
    row = iota(shape, 0)
    pick = iota(shape, 1) // 2 == 2 * lax.rem(row, n) + row // n
    pick = jnp.where(pick, 1.0, 0.0).astype(F32)
    for yg in range(3):
        both = jnp.concatenate(
            [RM[pl.ds(zl * 3 + yg, n, stride=8), :] for zl in range(2)], axis=0
        )
        wide = t_dot(both, pick)
        for y in range(4):
            for k in range(2):
                MQ[pl.ds(((yg * 4 + y) * 2 + k) * 32, 32), :] = wide[y * 32:(y + 1) * 32]

    even_y = lax.rem(iota((24, L), 0), 2) == 0
    even_z = lax.rem(iota((24, L), 1), 2) == 0

    def fine_speed(x8):
        mass = MQ[pl.ds(x8, 24, stride=32), :]
        inverse = SPEED_UNIT * 0.5 / mass
        out = []
        for c in range(3):
            s = SP[c * 8 + x8]
            s = s + jnp.where(even_y, pltpu.roll(s, 23, 0), pltpu.roll(s, 1, 0))
            s = s + jnp.where(even_z, turn(s, -1), turn(s, 1))
            m = MQ[pl.ds((c + 1) * 8 + x8, 24, stride=32), :]
            out.append((m + 0.5 * s) * inverse)
        return out

    def advance(src, e, r0, p, rows, speed):
        mid = src[e, pl.ds(r0, rows), :]
        advect = (
            speed[0] * (src[e + 1, pl.ds(r0, rows), :] - src[e - 1, pl.ds(r0, rows), :])
            + speed[1] * (src[e, pl.ds(r0 + 1, rows), :] - src[e, pl.ds(r0 - 1, rows), :])
            + speed[2] * (turn(mid, -1) - turn(mid, 1))
        )
        return mid + TIME_STEP * (lap(PT, p, 1, rows)[1] - advect)

    for x8 in range(8):
        speed = fine_speed(x8)
        if 2 <= x8 <= 5:
            for c in range(3):
                SP[c * 8 + x8] = speed[c]
        for d in (2 * x8 - 1, 2 * x8):
            if 0 <= d < 14:
                E1[d, pl.ds(4, 24), :] = advance(E, d + 4, 4, d + 2, 24, speed)

    potential(E1, 10, 6, 24)
    for x in range(4):
        speed = [SP[c * 8 + x + 2, pl.ds(4, 16), :] for c in range(3)]
        for k in (2 * x, 2 * x + 1):
            OD[k] = advance(E1, k + 3, 8, k + 1, 16, speed)

    @pl.loop(1, n)
    def _(k):
        frm = lax.rem(gy + k, n)
        force_copy(frm, frm, frm).wait_recv()

    half = n // 2
    expand = jnp.where(iota((half, L), 1) // 8 == iota((half, L), 0), 1.0, 0.0).astype(F32)
    for slot in range(5):
        whole = RF[pl.ds(slot, n, stride=8), :]
        for h in range(2):
            q = t_dot(whole[h * half:(h + 1) * half], expand)
            value = q[0:16]
            for y in range(1, 8):
                value = jnp.where(lax.rem(lane, 8) == y, q[y * 16:(y + 1) * 16], value)
            if slot < 4:
                FR[h, pl.ds(slot, 16, stride=4), :] = value
            else:
                FR[h, pl.ds(64, 16), :] = value

    state = []
    for h in range(2):
        mass = EP[h, MASS]
        inverse = 1.0 / mass
        force = [FR[h, pl.ds(c * 24, 24), :] for c in range(3)]
        flow = [(EP[h, MASS + 1 + c] + 0.5 * force[c]) * inverse for c in range(3)]
        square = flow[0] * flow[0] + flow[1] * flow[1] + flow[2] * flow[2]
        work = flow[0] * force[0] + flow[1] * force[1] + flow[2] * force[2]
        state.append((mass, force, flow, 1.0 - 1.5 * square, work))
    rate = 1.0 / RELAX_TIME
    gain = 1.0 - 0.5 / RELAX_TIME

    def along(speed, vector):
        out = None
        for c in range(3):
            if speed[c] == 1:
                out = vector[c] if out is None else out + vector[c]
            elif speed[c] == -1:
                out = -vector[c] if out is None else out - vector[c]
        return out

    for member in range(19):
        cx, cy, cz = SPEEDS[member]
        w = WEIGHTS[member]
        parts = []
        for h in range(2):
            mass, force, flow, rest, work = state[h]
            p = EP[h, member]
            if member == 0:
                new = (rate * w) * mass * rest - (3.0 * gain * w) * work
            else:
                cu, cf = along(SPEEDS[member], flow), along(SPEEDS[member], force)
                new = (rate * w) * mass * (rest + cu * (3.0 + 4.5 * cu)) + (gain * w) * (
                    3.0 * (cf - work) + 9.0 * cu * cf
                )
            parts.append(p * (1.0 - rate) + new)
        if cy:
            turned = [pltpu.roll(v, cy % L, 1) for v in parts]
            edge = lane == (0 if cy == 1 else L - 1)
            parts = [jnp.where(edge, turned[1 - h], turned[h]) for h in range(2)]
        for h in range(2):
            RS[member, h] = parts[h]
            for x in range(4):
                OP[member, x, :, pl.ds(h * L, L)] = RS[
                    member, h, pl.ds((x + 1 - cx) * 4 + 1 - cz, 2), :
                ]

    for copy in halo + face_x + face_z + edges:
        copy.wait_send()

    @pl.loop(1, n)
    def _(k):
        to = lax.rem(gy + k, n)
        moment_copy(to, to, gy).wait_send()
        force_copy(to, to, gy).wait_send()


def put(dens, pops, dens_out, pops_out, dsem, psem):
    first = pltpu.make_async_copy(dens, dens_out, dsem)
    second = pltpu.make_async_copy(pops, pops_out, psem)
    second.start()
    first.start()
    first.wait()
    second.wait()


def solution(mesh):
    nx, n = mesh.shape["gx"], mesh.shape["gy"]
    L = 4 * n

    def local(density, populations):
        vmem = lambda *shape: pltpu.VMEM(shape, F32)
        dma = lambda *shape: pltpu.SemaphoreType.DMA(shape)
        any_spec = pl.BlockSpec(memory_space=pl.ANY)
        vmem_spec = pl.BlockSpec(memory_space=pltpu.VMEM)
        shapes = (
            jax.ShapeDtypeStruct((8, 16, L), F32),
            jax.ShapeDtypeStruct((19, 4, 2, 2 * L), F32),
        )
        density = pltpu.with_memory_space_constraint(density, pltpu.HBM)
        populations = pltpu.with_memory_space_constraint(populations, pltpu.HBM)
        density, populations = pl.pallas_call(
            lambda *refs: kernel(nx, n, *refs),
            out_shape=shapes,
            in_specs=[any_spec, any_spec],
            out_specs=(vmem_spec, vmem_spec),
            scratch_shapes=[
                vmem(22, 40, L), vmem(14, 32, L), vmem(20, 40, L), vmem(18, 32, L),
                vmem(256, L), vmem(256, L), vmem(24, 24, L),
                vmem(n * 8, 128), vmem(n * 8, 128), vmem(n * 8, 128), vmem(n * 8, 128),
                vmem(768, L), vmem(2, 2, 32, L), vmem(19, 4, 2, 2 * L),
                vmem(2, FIELDS, 24, L), vmem(2, 26, 2, L), vmem(2, 26, 2, L),
                vmem(2, 18, 4, L), vmem(2, 18, 4, L), vmem(4, 16, L), vmem(4, 16, L),
                vmem(2, 80, L), vmem(19, 2, 24, L),
                dma(), dma(),
                dma(2), dma(2), dma(2), dma(2), dma(4), dma(4),
                dma(2), dma(2), dma(2), dma(2), dma(4), dma(4),
                dma(n), dma(n), dma(n), dma(n),
            ],
            compiler_params=pltpu.CompilerParams(
                collective_id=0, has_side_effects=True, vmem_limit_bytes=16 * 2**20
            ),
        )(density, populations)
        return pl.pallas_call(
            put,
            out_shape=shapes,
            in_specs=[any_spec, any_spec],
            out_specs=(any_spec, any_spec),
            scratch_shapes=[dma(), dma()],
            compiler_params=pltpu.CompilerParams(vmem_limit_bytes=8 * 2**20),
        )(density, populations)

    return jax.shard_map(
        local,
        mesh=mesh,
        in_specs=(P("gx", "gy", None), P(None, "gx", "gy", None)),
        out_specs=(P("gx", "gy", None), P(None, "gx", "gy", None)),
        check_vma=False,
    )
```

```python
import jax
import jax.numpy as jnp
from jax import lax
from jax.experimental import pallas as pl
from jax.experimental.pallas import tpu as pltpu
from jax.sharding import PartitionSpec as P

MESH = pl.DeviceIdType.MESH
EXACT = lax.Precision.HIGHEST
F32 = jnp.float32

TIME_STEP = 0.0008
FORCE_UNIT = 0.005
SPEED_UNIT = 2000.0
RELAX_TIME = 0.8
QUENCH = -0.25

SPEEDS = [
    (0, 0, 0),
    (1, 0, 0), (-1, 0, 0), (0, 1, 0), (0, -1, 0), (0, 0, 1), (0, 0, -1),
    (1, 1, 0), (-1, -1, 0), (1, -1, 0), (-1, 1, 0),
    (1, 0, 1), (-1, 0, -1), (1, 0, -1), (-1, 0, 1),
    (0, 1, 1), (0, -1, -1), (0, 1, -1), (0, -1, 1),
]
WEIGHTS = [1.0 / 3.0] + [1.0 / 18.0] * 6 + [1.0 / 36.0] * 12

MASS = 19
FIELDS = 23
RISE_X = [q for q in range(19) if SPEEDS[q][0] == 1]
FALL_X = [q for q in range(19) if SPEEDS[q][0] == -1]
RISE_Z = [q for q in range(19) if SPEEDS[q][2] == 1]
FALL_Z = [q for q in range(19) if SPEEDS[q][2] == -1]
MOMENTS = [MASS, MASS + 1, MASS + 2, MASS + 3]
DIAGONALS = [(1, 1), (1, -1), (-1, 1), (-1, -1)]


def dot_t(a, b):
    return lax.dot_general(
        a, b, (((1,), (1,)), ((), ())), precision=EXACT, preferred_element_type=F32
    )


def t_dot(a, b):
    return lax.dot_general(
        a, b, (((0,), (0,)), ((), ())), precision=EXACT, preferred_element_type=F32
    )


def iota(shape, dim):
    return lax.broadcasted_iota(jnp.int32, shape, dim)


def kernel(
    nx, n, dens_hbm, pops_hbm, OD, OP,
    E, E2, E1, L1, PT, FA, FB, SP, SF, RF, SM, RM, MQ, MX, PV, EP, XS, XR, ZS, ZR, DS, DR, FR, RS,
    dsem, psem, h1_s, h1_r, h2_s, h2_r, px_s, px_r, pz_s, pz_r, pd_s, pd_r,
    ms_s, ms_r, fs_s, fs_r,
):
    L = 4 * n
    gx = lax.axis_index("gx")
    gy = lax.axis_index("gy")

    def place(sx, sy):
        return {"gx": lax.rem(gx + sx + nx, nx), "gy": lax.rem(gy + sy + n, n)}

    barrier = pltpu.get_barrier_semaphore()
    for sx, sy in DIAGONALS + [(1, 0), (-1, 0)]:
        pl.semaphore_signal(barrier, inc=1, device_id=place(sx, sy), device_id_type=MESH)

    @pl.loop(1, n)
    def _(k):
        pl.semaphore_signal(barrier, inc=1, device_id=place(0, k), device_id_type=MESH)

    dens_in = pltpu.make_async_copy(dens_hbm, E.at[pl.ds(5, 8), pl.ds(8, 16)], dsem)
    dens_in.start()
    pops_in = pltpu.make_async_copy(pops_hbm, PV, psem)
    pops_in.start()

    def remote(src, dst, send, recv, where):
        return pltpu.make_async_remote_copy(
            src_ref=src, dst_ref=dst, send_sem=send, recv_sem=recv, device_id=where,
            device_id_type=MESH,
        )

    dens_in.wait()
    pl.semaphore_wait(barrier, n + 5)

    def boxes(items, target, send, recv):
        return [
            remote(
                E.at[pl.ds(x0, xs), pl.ds(y0, ys)], target.at[pl.ds(x1, xs), pl.ds(y1, ys)],
                send.at[i], recv.at[i], place(*where),
            )
            for i, (where, x0, x1, xs, y0, y1, ys) in enumerate(items)
        ]

    halo = boxes(
        [
            ((sx, sy), *((9, 1, 4) if sx == 1 else (5, 13, 4)),
             *((21, 5, 3) if sy == 1 else (8, 24, 3)))
            for sx, sy in DIAGONALS
        ] + [
            ((1, 0), 8, 0, 5, 8, 8, 16),
            ((-1, 0), 5, 13, 5, 8, 8, 16),
            ((0, 1), 5, 5, 8, 21, 5, 3),
            ((0, -1), 5, 5, 8, 8, 24, 3),
        ],
        E, h1_s, h1_r,
    )
    for copy in halo:
        copy.start()

    lane = iota((1, L), 1)

    pops_in.wait()
    for h in range(2):
        for member in range(19):
            for x in range(4):
                EP[h, member, pl.ds(x * 4 + 5, 2), :] = PV[member, x, :, pl.ds(h * L, L)]
        total = jnp.zeros((24, L), F32)
        moment = [jnp.zeros((24, L), F32) for _ in range(3)]
        for member in range(19):
            value = EP[h, member]
            total = total + value
            for c in range(3):
                if SPEEDS[member][c] == 1:
                    moment[c] = moment[c] + value
                elif SPEEDS[member][c] == -1:
                    moment[c] = moment[c] - value
        EP[h, MASS] = total
        for c in range(3):
            EP[h, MASS + 1 + c] = moment[c]

    for way, (members, row, rows) in enumerate(
        ((RISE_X, 17, (13, 17)), (FALL_X, 5, (5, 9)))
    ):
        for h in range(2):
            for f in range(5):
                XS[way, f * 2 + h] = EP[h, members[f], pl.ds(row, 2), :]
            for c in range(4):
                for layer in range(2):
                    XS[way, 10 + (c * 2 + layer) * 2 + h] = EP[
                        h, MASS + c, pl.ds(rows[layer], 2), :
                    ]
    face_x = [
        remote(XS.at[0], XR.at[0], px_s.at[0], px_r.at[0], place(1, 0)),
        remote(XS.at[1], XR.at[1], px_s.at[1], px_r.at[1], place(-1, 0)),
    ]
    for copy in face_x:
        copy.start()

    outer = boxes(
        [
            ((1, 0), 6, 0, 2, 8, 8, 16),
            ((-1, 0), 10, 20, 2, 8, 8, 16),
            ((0, 1), 5, 7, 8, 17, 1, 4),
            ((0, -1), 5, 7, 8, 11, 27, 4),
        ] + [
            ((sx, sy), *((10, 4, 3) if sx == 1 else (5, 15, 3)),
             *((18, 2, 3) if sy == 1 else (11, 27, 3)))
            for sx, sy in DIAGONALS
        ] + [
            ((sx, sy), *((7, 1, 2) if sx == 1 else (9, 19, 2)),
             *((22, 6, 2) if sy == 1 else (8, 24, 2)))
            for sx, sy in DIAGONALS
        ],
        E2, h2_s, h2_r,
    )
    for copy in outer:
        copy.start()

    for way, (members, zi) in enumerate(((RISE_Z, 2), (FALL_Z, 1))):
        for f, field in enumerate(members + MOMENTS):
            for h in range(2):
                ZS[way, f * 2 + h] = EP[h, field, pl.ds(4 + zi, 4, stride=4), :]
    face_z = [
        remote(ZS.at[0], ZR.at[0], pz_s.at[0], pz_r.at[0], place(0, 1)),
        remote(ZS.at[1], ZR.at[1], pz_s.at[1], pz_r.at[1], place(0, -1)),
    ]
    for copy in face_z:
        copy.start()

    for h in range(2):
        for zl in range(2):
            for c in range(4):
                MX[zl, h, pl.ds(c * 8 + 2, 4), :] = EP[h, MASS + c, pl.ds(5 + zl, 4, stride=4), :]
    for way in range(2):
        face_x[way].wait_recv()
        for h in range(2):
            for c in range(4):
                for layer in range(2):
                    both = XR[way, 10 + (c * 2 + layer) * 2 + h]
                    for zl in range(2):
                        MX[zl, h, pl.ds(c * 8 + way * 6 + layer, 1), :] = both[zl:zl + 1]
    shape = (3 * n, L)
    row, col = iota(shape, 0), iota(shape, 1)
    spread = []
    for h in range(2):
        t = lax.rem(col + (h * L + 2 + 8 * n) - 4 * (row // n), 8 * n)
        hit = jnp.logical_and(t // 8 == lax.rem(row, n), lax.rem(t, 8) < 4)
        spread.append(jnp.where(hit, 1.0, 0.0).astype(F32))
    for zl in range(2):
        result = None
        for h in range(2):
            values = MX[zl, h]
            tiles = jnp.concatenate(
                [jnp.where(lax.rem(lane + 2, 4) == y, values, 0.0) for y in range(4)], axis=0
            )
            part = dot_t(spread[h], tiles)
            result = part if result is None else result + part
        for yg in range(3):
            SM[pl.ds(zl * 3 + yg, n, stride=8), :] = result[yg * n:(yg + 1) * n]

    def moment_copy(to, sem_to, slot):
        return remote(
            SM.at[pl.ds(pl.multiple_of(to * 8, 8), 6)],
            RM.at[pl.ds(pl.multiple_of(slot * 8, 8), 6)],
            ms_s.at[sem_to], ms_r.at[slot], {"gx": gx, "gy": to},
        )

    def force_copy(to, sem_to, slot):
        return remote(
            SF.at[pl.ds(pl.multiple_of(to * 8, 8), 5)],
            RF.at[pl.ds(pl.multiple_of(slot * 8, 8), 5)],
            fs_s.at[sem_to], fs_r.at[slot], {"gx": gx, "gy": to},
        )

    @pl.loop(1, n)
    def _(k):
        to = lax.rem(gy + k, n)
        moment_copy(to, to, gy).start()

    for slot in range(6):
        RM[pl.ds(gy * 8 + slot, 1), :] = SM[pl.ds(gy * 8 + slot, 1), :]

    for way in range(2):
        for side, (members, layer) in enumerate(((RISE_X, 1), (FALL_X, 0))):
            member = SPEEDS.index((1 - 2 * side, 0, 1 - 2 * way))
            picks = [members.index(member)] + [5 + c * 2 + layer for c in range(4)]
            for f, item in enumerate(picks):
                for h in range(2):
                    both = XR[side, item * 2 + h]
                    DS[way, pl.ds((side * 5 + f) * 2 + h, 1), :] = both[1 - way:2 - way]
    edges = [
        remote(DS.at[0], DR.at[0], pd_s.at[0], pd_r.at[0], place(0, 1)),
        remote(DS.at[1], DR.at[1], pd_s.at[1], pd_r.at[1], place(0, -1)),
    ]
    for copy in edges:
        copy.start()

    for way, (members, row, layer) in enumerate(((RISE_X, 1, 1), (FALL_X, 21, 0))):
        for h in range(2):
            for f in range(5):
                EP[h, members[f], pl.ds(row, 2), :] = XR[way, f * 2 + h]
            for c in range(4):
                EP[h, MASS + c, pl.ds(row, 2), :] = XR[way, 10 + (c * 2 + layer) * 2 + h]

    def turn(value, by):
        return pltpu.roll(value, by % L, 1)

    def lap(ref, i, r0, rows):
        c = ref[i, pl.ds(r0, rows), :]
        return c, (
            -6.0 * c + ref[i - 1, pl.ds(r0, rows), :] + ref[i + 1, pl.ds(r0, rows), :]
            + ref[i, pl.ds(r0 - 1, rows), :] + ref[i, pl.ds(r0 + 1, rows), :]
            + turn(c, 1) + turn(c, -1)
        )

    def potential(src, first, layers, r0, rows):
        for i in range(layers + 2):
            L1[i, pl.ds(0, rows), :] = lap(src, first + i + 1, r0, rows)[1]
        for j in range(layers):
            c, second = lap(L1, j + 1, 1, rows)
            rho = src[first + j + 2, pl.ds(r0 + 1, rows), :]
            PT[j, pl.ds(0, rows), :] = (
                (QUENCH + 1.0) * rho + 2.0 * c + second + rho * rho * rho
            )

    for copy in halo:
        copy.wait_recv()
    potential(E, 0, 14, 6, 24)

    scale = -0.5 * FORCE_UNIT * 0.125
    zeros = jnp.zeros((16, L), F32)
    for extra in range(8, 16):
        FB[pl.ds(extra, 16, stride=16), :] = zeros

    def force_pair(src, e0, p0, r0, rows):
        sums = [None, None, None]
        for k in range(2):
            rho = src[e0 + k, pl.ds(r0, rows), :] * scale
            mid = PT[p0 + k, pl.ds(1, rows), :]
            parts = (
                PT[p0 + k + 1, pl.ds(1, rows), :] - PT[p0 + k - 1, pl.ds(1, rows), :],
                PT[p0 + k, pl.ds(2, rows), :] - PT[p0 + k, pl.ds(0, rows), :],
                turn(mid, -1) - turn(mid, 1),
            )
            for c in range(3):
                value = rho * parts[c]
                sums[c] = value if sums[c] is None else sums[c] + value
        return sums

    for xi in range(6):
        sums = force_pair(E, 2 * xi + 3, 2 * xi + 1, 8, 16)
        for c in range(3):
            cx = c * 6 + xi
            if cx < 16:
                FA[pl.ds(cx, 16, stride=16), :] = sums[c]
            else:
                for zl in range(4):
                    FB[pl.ds((cx - 16) * 4 + zl, 16, stride=16), :] = turn(
                        sums[c], -2 * (zl - 1)
                    )
    shape = (4 * n, L)
    row = iota(shape, 0)
    window = lax.rem(2 * lax.rem(row, n) - 1 + row // n + 2 * n, 2 * n)
    choose = jnp.where(iota(shape, 1) // 2 == window, 1.0, 0.0).astype(F32)
    ga = jnp.concatenate(
        [FA[pl.ds(32 * y, 16), :] + FA[pl.ds(32 * y + 16, 16), :] for y in range(8)], axis=0
    )
    gb = jnp.concatenate(
        [FB[pl.ds(32 * y, 16), :] + FB[pl.ds(32 * y + 16, 16), :] for y in range(8)], axis=0
    )
    ta = dot_t(choose, ga)
    tb = dot_t(choose[n:2 * n], gb)
    for zl in range(4):
        SF[pl.ds(zl, n, stride=8), :] = ta[zl * n:(zl + 1) * n]
    SF[pl.ds(4, n, stride=8), :] = tb

    @pl.loop(1, n)
    def _(k):
        to = lax.rem(gy + k, n)
        force_copy(to, to, gy).start()

    for slot in range(5):
        RF[pl.ds(gy * 8 + slot, 1), :] = SF[pl.ds(gy * 8 + slot, 1), :]

    for way, (members, zi) in enumerate(((RISE_Z, 0), (FALL_Z, 3))):
        face_z[way].wait_recv()
        for f, field in enumerate(members + MOMENTS):
            for h in range(2):
                EP[h, field, pl.ds(4 + zi, 4, stride=4), :] = ZR[way, f * 2 + h]

    for copy in outer:
        copy.wait_recv()
    for e in range(18):
        y0, ys = (8, 16) if e in (0, 17) else (5, 22)
        E2[e + 2, pl.ds(y0, ys), :] = E[e, pl.ds(y0, ys), :]
    potential(E2, 0, 18, 2, 32)
    for x8 in range(8):
        sums = force_pair(E2, 2 * x8 + 3, 2 * x8 + 1, 4, 24)
        for c in range(3):
            SP[c * 8 + x8] = sums[c]

    @pl.loop(1, n)
    def _(k):
        frm = lax.rem(gy + k, n)
        moment_copy(frm, frm, frm).wait_recv()

    shape = (2 * n, L)
    row = iota(shape, 0)
    pick = iota(shape, 1) // 2 == 2 * lax.rem(row, n) + row // n
    pick = jnp.where(pick, 1.0, 0.0).astype(F32)
    for yg in range(3):
        both = jnp.concatenate(
            [RM[pl.ds(zl * 3 + yg, n, stride=8), :] for zl in range(2)], axis=0
        )
        wide = t_dot(both, pick)
        for y in range(4):
            for k in range(2):
                MQ[pl.ds(((yg * 4 + y) * 2 + k) * 32, 32), :] = wide[y * 32:(y + 1) * 32]

    even_y = lax.rem(iota((24, L), 0), 2) == 0
    even_z = lax.rem(iota((24, L), 1), 2) == 0

    def fine_speed(x8):
        mass = MQ[pl.ds(x8, 24, stride=32), :]
        inverse = SPEED_UNIT * 0.5 / mass
        out = []
        for c in range(3):
            s = SP[c * 8 + x8]
            s = s + jnp.where(even_y, pltpu.roll(s, 23, 0), pltpu.roll(s, 1, 0))
            s = s + jnp.where(even_z, turn(s, -1), turn(s, 1))
            m = MQ[pl.ds((c + 1) * 8 + x8, 24, stride=32), :]
            out.append((m + 0.5 * s) * inverse)
        return out

    def advance(src, e, r0, p, rows, speed):
        mid = src[e, pl.ds(r0, rows), :]
        advect = (
            speed[0] * (src[e + 1, pl.ds(r0, rows), :] - src[e - 1, pl.ds(r0, rows), :])
            + speed[1] * (src[e, pl.ds(r0 + 1, rows), :] - src[e, pl.ds(r0 - 1, rows), :])
            + speed[2] * (turn(mid, -1) - turn(mid, 1))
        )
        return mid + TIME_STEP * (lap(PT, p, 1, rows)[1] - advect)

    for x8 in range(8):
        speed = fine_speed(x8)
        if 2 <= x8 <= 5:
            for c in range(3):
                SP[c * 8 + x8] = speed[c]
        for d in (2 * x8 - 1, 2 * x8):
            if 0 <= d < 14:
                E1[d, pl.ds(4, 24), :] = advance(E2, d + 4, 4, d + 2, 24, speed)

    potential(E1, 0, 10, 6, 24)
    for x in range(4):
        speed = [SP[c * 8 + x + 2, pl.ds(4, 16), :] for c in range(3)]
        for k in (2 * x, 2 * x + 1):
            OD[k] = advance(E1, k + 3, 8, k + 1, 16, speed)

    for way in range(2):
        edges[way].wait_recv()
        for side in range(2):
            row = side * 20 + way * 3
            member = SPEEDS.index((1 - 2 * side, 0, 1 - 2 * way))
            for f, field in enumerate([member] + MOMENTS):
                for h in range(2):
                    EP[h, field, pl.ds(row, 1), :] = DR[way, pl.ds((side * 5 + f) * 2 + h, 1), :]

    @pl.loop(1, n)
    def _(k):
        frm = lax.rem(gy + k, n)
        force_copy(frm, frm, frm).wait_recv()

    half = n // 2
    expand = jnp.where(iota((half, L), 1) // 8 == iota((half, L), 0), 1.0, 0.0).astype(F32)
    for slot in range(5):
        whole = RF[pl.ds(slot, n, stride=8), :]
        for h in range(2):
            q = t_dot(whole[h * half:(h + 1) * half], expand)
            value = q[0:16]
            for y in range(1, 8):
                value = jnp.where(lax.rem(lane, 8) == y, q[y * 16:(y + 1) * 16], value)
            if slot < 4:
                FR[h, pl.ds(slot, 16, stride=4), :] = value
            else:
                FR[h, pl.ds(64, 16), :] = value

    state = []
    for h in range(2):
        mass = EP[h, MASS]
        inverse = 1.0 / mass
        force = [FR[h, pl.ds(c * 24, 24), :] for c in range(3)]
        flow = [(EP[h, MASS + 1 + c] + 0.5 * force[c]) * inverse for c in range(3)]
        square = flow[0] * flow[0] + flow[1] * flow[1] + flow[2] * flow[2]
        work = flow[0] * force[0] + flow[1] * force[1] + flow[2] * force[2]
        state.append((mass, force, flow, 1.0 - 1.5 * square, work))
    rate = 1.0 / RELAX_TIME
    gain = 1.0 - 0.5 / RELAX_TIME

    def along(speed, vector):
        out = None
        for c in range(3):
            if speed[c] == 1:
                out = vector[c] if out is None else out + vector[c]
            elif speed[c] == -1:
                out = -vector[c] if out is None else out - vector[c]
        return out

    for member in range(19):
        cx, cy, cz = SPEEDS[member]
        w = WEIGHTS[member]
        parts = []
        for h in range(2):
            mass, force, flow, rest, work = state[h]
            p = EP[h, member]
            if member == 0:
                new = (rate * w) * mass * rest - (3.0 * gain * w) * work
            else:
                cu, cf = along(SPEEDS[member], flow), along(SPEEDS[member], force)
                new = (rate * w) * mass * (rest + cu * (3.0 + 4.5 * cu)) + (gain * w) * (
                    3.0 * (cf - work) + 9.0 * cu * cf
                )
            parts.append(p * (1.0 - rate) + new)
        if cy:
            turned = [pltpu.roll(v, cy % L, 1) for v in parts]
            edge = lane == (0 if cy == 1 else L - 1)
            parts = [jnp.where(edge, turned[1 - h], turned[h]) for h in range(2)]
        for h in range(2):
            RS[member, h] = parts[h]
            for x in range(4):
                OP[member, x, :, pl.ds(h * L, L)] = RS[
                    member, h, pl.ds((x + 1 - cx) * 4 + 1 - cz, 2), :
                ]

    for copy in halo + outer + face_x + face_z + edges:
        copy.wait_send()

    @pl.loop(1, n)
    def _(k):
        to = lax.rem(gy + k, n)
        moment_copy(to, to, gy).wait_send()
        force_copy(to, to, gy).wait_send()


def put(dens, pops, dens_out, pops_out, dsem, psem):
    first = pltpu.make_async_copy(dens, dens_out, dsem)
    second = pltpu.make_async_copy(pops, pops_out, psem)
    second.start()
    first.start()
    first.wait()
    second.wait()


def solution(mesh):
    nx, n = mesh.shape["gx"], mesh.shape["gy"]
    L = 4 * n

    def local(density, populations):
        vmem = lambda *shape: pltpu.VMEM(shape, F32)
        dma = lambda *shape: pltpu.SemaphoreType.DMA(shape)
        any_spec = pl.BlockSpec(memory_space=pl.ANY)
        vmem_spec = pl.BlockSpec(memory_space=pltpu.VMEM)
        shapes = (
            jax.ShapeDtypeStruct((8, 16, L), F32),
            jax.ShapeDtypeStruct((19, 4, 2, 2 * L), F32),
        )
        density = pltpu.with_memory_space_constraint(density, pltpu.HBM)
        populations = pltpu.with_memory_space_constraint(populations, pltpu.HBM)
        density, populations = pl.pallas_call(
            lambda *refs: kernel(nx, n, *refs),
            out_shape=shapes,
            in_specs=[any_spec, any_spec],
            out_specs=(vmem_spec, vmem_spec),
            scratch_shapes=[
                vmem(18, 32, L), vmem(22, 40, L), vmem(14, 32, L),
                vmem(20, 40, L), vmem(18, 32, L),
                vmem(256, L), vmem(256, L), vmem(24, 24, L),
                vmem(n * 8, 128), vmem(n * 8, 128), vmem(n * 8, 128), vmem(n * 8, 128),
                vmem(768, L), vmem(2, 2, 32, L), vmem(19, 4, 2, 2 * L),
                vmem(2, FIELDS, 24, L), vmem(2, 26, 2, L), vmem(2, 26, 2, L),
                vmem(2, 18, 4, L), vmem(2, 18, 4, L), vmem(2, 24, L), vmem(2, 24, L),
                vmem(2, 80, L), vmem(19, 2, 24, L),
                dma(), dma(),
                dma(8), dma(8), dma(12), dma(12),
                dma(2), dma(2), dma(2), dma(2), dma(2), dma(2),
                dma(n), dma(n), dma(n), dma(n),
            ],
            compiler_params=pltpu.CompilerParams(
                collective_id=0, has_side_effects=True, vmem_limit_bytes=16 * 2**20
            ),
        )(density, populations)
        return pl.pallas_call(
            put,
            out_shape=shapes,
            in_specs=[any_spec, any_spec],
            out_specs=(any_spec, any_spec),
            scratch_shapes=[dma(), dma()],
            compiler_params=pltpu.CompilerParams(vmem_limit_bytes=8 * 2**20),
        )(density, populations)

    return jax.shard_map(
        local,
        mesh=mesh,
        in_specs=(P("gx", "gy", None), P(None, "gx", "gy", None)),
        out_specs=(P("gx", "gy", None), P(None, "gx", "gy", None)),
        check_vma=False,
    )
```

```python
import jax
import jax.numpy as jnp
from jax import lax
from jax.experimental import pallas as pl
from jax.experimental.pallas import tpu as pltpu
from jax.sharding import PartitionSpec as P

MESH = pl.DeviceIdType.MESH
EXACT = lax.Precision.HIGHEST
F32 = jnp.float32

TIME_STEP = 0.0008
FORCE_UNIT = 0.005
SPEED_UNIT = 2000.0
RELAX_TIME = 0.8
QUENCH = -0.25

SPEEDS = [
    (0, 0, 0),
    (1, 0, 0), (-1, 0, 0), (0, 1, 0), (0, -1, 0), (0, 0, 1), (0, 0, -1),
    (1, 1, 0), (-1, -1, 0), (1, -1, 0), (-1, 1, 0),
    (1, 0, 1), (-1, 0, -1), (1, 0, -1), (-1, 0, 1),
    (0, 1, 1), (0, -1, -1), (0, 1, -1), (0, -1, 1),
]
WEIGHTS = [1.0 / 3.0] + [1.0 / 18.0] * 6 + [1.0 / 36.0] * 12

MASS = 19
FIELDS = 23
RISE_X = [q for q in range(19) if SPEEDS[q][0] == 1]
FALL_X = [q for q in range(19) if SPEEDS[q][0] == -1]
RISE_Z = [q for q in range(19) if SPEEDS[q][2] == 1]
FALL_Z = [q for q in range(19) if SPEEDS[q][2] == -1]
MOMENTS = [MASS, MASS + 1, MASS + 2, MASS + 3]
DIAGONALS = [(1, 1), (1, -1), (-1, 1), (-1, -1)]


def dot_t(a, b):
    return lax.dot_general(
        a, b, (((1,), (1,)), ((), ())), precision=EXACT, preferred_element_type=F32
    )


def t_dot(a, b):
    return lax.dot_general(
        a, b, (((0,), (0,)), ((), ())), precision=EXACT, preferred_element_type=F32
    )


def iota(shape, dim):
    return lax.broadcasted_iota(jnp.int32, shape, dim)


def kernel(
    nx, n, dens_hbm, pops_hbm, OD, OP,
    E, E1, L1, PT, FA, FB, SP, SF, RF, SM, RM, MQ, MX, PV, EP, XS, XR, ZS, ZR, DS, DR, FR, RS,
    dsem, psem, h1_s, h1_r, h2_s, h2_r, px_s, px_r, pz_s, pz_r, pd_s, pd_r,
    ms_s, ms_r, fs_s, fs_r,
):
    L = 4 * n
    gx = lax.axis_index("gx")
    gy = lax.axis_index("gy")

    def place(sx, sy):
        return {"gx": lax.rem(gx + sx + nx, nx), "gy": lax.rem(gy + sy + n, n)}

    barrier = pltpu.get_barrier_semaphore()
    for sx, sy in DIAGONALS + [(1, 0), (-1, 0)]:
        pl.semaphore_signal(barrier, inc=1, device_id=place(sx, sy), device_id_type=MESH)

    @pl.loop(1, n)
    def _(k):
        pl.semaphore_signal(barrier, inc=1, device_id=place(0, k), device_id_type=MESH)

    dens_in = pltpu.make_async_copy(dens_hbm, E.at[pl.ds(5, 8), pl.ds(8, 16)], dsem)
    dens_in.start()
    pops_in = pltpu.make_async_copy(pops_hbm, PV, psem)
    pops_in.start()

    def remote(src, dst, send, recv, where):
        return pltpu.make_async_remote_copy(
            src_ref=src, dst_ref=dst, send_sem=send, recv_sem=recv, device_id=where,
            device_id_type=MESH,
        )

    lane = iota((1, L), 1)

    pops_in.wait()
    for h in range(2):
        for member in range(19):
            for x in range(4):
                EP[h, member, pl.ds(x * 4 + 5, 2), :] = PV[member, x, :, pl.ds(h * L, L)]
        total = jnp.zeros((24, L), F32)
        moment = [jnp.zeros((24, L), F32) for _ in range(3)]
        for member in range(19):
            value = EP[h, member]
            total = total + value
            for c in range(3):
                if SPEEDS[member][c] == 1:
                    moment[c] = moment[c] + value
                elif SPEEDS[member][c] == -1:
                    moment[c] = moment[c] - value
        EP[h, MASS] = total
        for c in range(3):
            EP[h, MASS + 1 + c] = moment[c]

    for way, (members, row) in enumerate(((RISE_X, 17), (FALL_X, 5))):
        for f, field in enumerate(members + MOMENTS):
            for h in range(2):
                XS[way, f * 2 + h] = EP[h, field, pl.ds(row, 2), :]
    for way, (members, zi) in enumerate(((RISE_Z, 2), (FALL_Z, 1))):
        for f, field in enumerate(members + MOMENTS):
            for h in range(2):
                ZS[way, f * 2 + h] = EP[h, field, pl.ds(4 + zi, 4, stride=4), :]
    spread = [
        jnp.where((iota((n, L), 1) + h * L) // 8 == iota((n, L), 0), 1.0, 0.0).astype(F32)
        for h in range(2)
    ]
    for zl in range(2):
        result = None
        for h in range(2):
            for c in range(4):
                MX[zl, h, pl.ds(c * 4, 4), :] = EP[h, MASS + c, pl.ds(5 + zl, 4, stride=4), :]
            values = MX[zl, h]
            tiles = jnp.concatenate(
                [jnp.where(lax.rem(lane, 8) == y, values, 0.0) for y in range(8)], axis=0
            )
            part = dot_t(spread[h], tiles)
            result = part if result is None else result + part
        SM[pl.ds(zl, n, stride=8), :] = result

    dens_in.wait()
    pl.semaphore_wait(barrier, n + 5)

    def boxes(buf, items, send, recv):
        copies = []
        for i, (where, x0, x1, xs, y0, y1, ys) in enumerate(items):
            copies.append(remote(
                buf.at[pl.ds(x0, xs), pl.ds(y0, ys)], buf.at[pl.ds(x1, xs), pl.ds(y1, ys)],
                send.at[i], recv.at[i], place(*where),
            ))
        for copy in copies:
            copy.start()
        return copies

    def around(width, corner, rows):
        lo, hi = width, width + 8
        return [
            ((sx, sy),
             *((hi - corner, lo - corner, corner) if sx == 1 else (lo, hi, corner)),
             *((24 - rows, 8 - rows, rows) if sy == 1 else (8, 24, rows)))
            for sx, sy in DIAGONALS
        ] + [
            ((1, 0), hi - width, 0, width, 8, 8, 16),
            ((-1, 0), lo, hi, width, 8, 8, 16),
            ((0, 1), lo, lo, 8, 21, 5, 3),
            ((0, -1), lo, lo, 8, 8, 24, 3),
        ]

    def others():
        if n % 32:
            return [lax.rem(gy + k, n) for k in range(1, n)]
        z, inner = gy // 8, lax.rem(gy, 8)
        groups = (3 - z, lax.rem(z + 2, 4), z + 1 - 2 * lax.rem(z, 2), z)
        return [
            to_z * 8 + lax.rem(inner + k, 8)
            for i, to_z in enumerate(groups) for k in range(1 if i == 3 else 0, 8)
        ]

    def to_all(src, dst, rows, send, recv):
        for to in others():
            remote(
                src.at[pl.ds(pl.multiple_of(to * 8, 8), rows)],
                dst.at[pl.ds(pl.multiple_of(gy * 8, 8), rows)],
                send, recv, {"gx": gx, "gy": to},
            ).start()
        for slot in range(rows):
            dst[pl.ds(gy * 8 + slot, 1), :] = src[pl.ds(gy * 8 + slot, 1), :]

    def wait_all(buf, rows, sem):
        whole = buf.at[pl.ds(0, (n - 1) * rows)]
        pltpu.make_async_copy(whole, whole, sem).wait()

    halo = boxes(E, around(5, 4, 3), h1_s, h1_r)
    to_all(SM, RM, 2, ms_s, ms_r)
    face_x = [
        remote(XS.at[0], XR.at[0], px_s.at[0], px_r.at[0], place(1, 0)),
        remote(XS.at[1], XR.at[1], px_s.at[1], px_r.at[1], place(-1, 0)),
    ]
    face_z = [
        remote(ZS.at[0], ZR.at[0], pz_s.at[0], pz_r.at[0], place(0, 1)),
        remote(ZS.at[1], ZR.at[1], pz_s.at[1], pz_r.at[1], place(0, -1)),
    ]
    for copy in face_x + face_z:
        copy.start()

    def turn(value, by):
        return pltpu.roll(value, by % L, 1)

    def lap(ref, i, r0, rows):
        c = ref[i, pl.ds(r0, rows), :]
        return c, (
            -6.0 * c + ref[i - 1, pl.ds(r0, rows), :] + ref[i + 1, pl.ds(r0, rows), :]
            + ref[i, pl.ds(r0 - 1, rows), :] + ref[i, pl.ds(r0 + 1, rows), :]
            + turn(c, 1) + turn(c, -1)
        )

    def potential(src, first, layers, r0, rows):
        for i in range(layers + 2):
            L1[i, pl.ds(0, rows), :] = lap(src, first + i + 1, r0, rows)[1]
        for j in range(layers):
            c, second = lap(L1, j + 1, 1, rows)
            rho = src[first + j + 2, pl.ds(r0 + 1, rows), :]
            PT[j, pl.ds(0, rows), :] = (
                (QUENCH + 1.0) * rho + 2.0 * c + second + rho * rho * rho
            )

    for copy in halo:
        copy.wait_recv()
    potential(E, 0, 14, 6, 24)

    scale = -0.5 * FORCE_UNIT * 0.125
    zeros = jnp.zeros((16, L), F32)
    for extra in range(8, 16):
        FB[pl.ds(extra, 16, stride=16), :] = zeros

    def force_pair(src, e0, p0, r0, rows):
        sums = [None, None, None]
        for k in range(2):
            rho = src[e0 + k, pl.ds(r0, rows), :] * scale
            mid = PT[p0 + k, pl.ds(1, rows), :]
            parts = (
                PT[p0 + k + 1, pl.ds(1, rows), :] - PT[p0 + k - 1, pl.ds(1, rows), :],
                PT[p0 + k, pl.ds(2, rows), :] - PT[p0 + k, pl.ds(0, rows), :],
                turn(mid, -1) - turn(mid, 1),
            )
            for c in range(3):
                value = rho * parts[c]
                sums[c] = value if sums[c] is None else sums[c] + value
        return sums

    for xi in range(6):
        sums = force_pair(E, 2 * xi + 3, 2 * xi + 1, 8, 16)
        for c in range(3):
            cx = c * 6 + xi
            if 1 <= xi <= 4:
                SP[c * 4 + xi - 1] = sums[c]
            if cx < 16:
                FA[pl.ds(cx, 16, stride=16), :] = sums[c]
            else:
                for zl in range(4):
                    FB[pl.ds((cx - 16) * 4 + zl, 16, stride=16), :] = turn(
                        sums[c], -2 * (zl - 1)
                    )
    shape = (4 * n, L)
    row = iota(shape, 0)
    window = lax.rem(2 * lax.rem(row, n) - 1 + row // n + 2 * n, 2 * n)
    choose = jnp.where(iota(shape, 1) // 2 == window, 1.0, 0.0).astype(F32)
    ga = jnp.concatenate(
        [FA[pl.ds(32 * y, 16), :] + FA[pl.ds(32 * y + 16, 16), :] for y in range(8)], axis=0
    )
    gb = jnp.concatenate(
        [FB[pl.ds(32 * y, 16), :] + FB[pl.ds(32 * y + 16, 16), :] for y in range(8)], axis=0
    )
    ta = dot_t(choose, ga)
    tb = dot_t(choose[n:2 * n], gb)
    for zl in range(4):
        SF[pl.ds(zl, n, stride=8), :] = ta[zl * n:(zl + 1) * n]
    SF[pl.ds(4, n, stride=8), :] = tb

    to_all(SF, RF, 5, fs_s, fs_r)

    wait_all(RM, 2, ms_r)
    shape = (2 * n, L)
    row = iota(shape, 0)
    pick = iota(shape, 1) // 2 == 2 * lax.rem(row, n) + row // n
    both = jnp.concatenate([RM[pl.ds(zl, n, stride=8), :] for zl in range(2)], axis=0)
    wide = t_dot(both, jnp.where(pick, 1.0, 0.0).astype(F32))
    for y in range(16):
        MQ[pl.ds(y * 16, 16), :] = wide[(y // 2) * 16:(y // 2 + 1) * 16]

    even_y = lax.rem(iota((16, L), 0), 2) == 0
    even_z = lax.rem(iota((16, L), 1), 2) == 0

    def fine_speed(x):
        mass = MQ[pl.ds(x, 16, stride=16), :]
        inverse = SPEED_UNIT * 0.5 / mass
        out = []
        for c in range(3):
            s = SP[c * 4 + x]
            s = s + jnp.where(even_y, pltpu.roll(s, 15, 0), pltpu.roll(s, 1, 0))
            s = s + jnp.where(even_z, turn(s, -1), turn(s, 1))
            m = MQ[pl.ds((c + 1) * 4 + x, 16, stride=16), :]
            out.append((m + 0.5 * s) * inverse)
        return out

    def advance(src, e, p, speed):
        mid = src[e, pl.ds(8, 16), :]
        advect = (
            speed[0] * (src[e + 1, pl.ds(8, 16), :] - src[e - 1, pl.ds(8, 16), :])
            + speed[1] * (src[e, pl.ds(9, 16), :] - src[e, pl.ds(7, 16), :])
            + speed[2] * (turn(mid, -1) - turn(mid, 1))
        )
        return mid + TIME_STEP * (lap(PT, p, 1, 16)[1] - advect)

    for x in range(4):
        speed = fine_speed(x)
        for c in range(3):
            SP[c * 4 + x] = speed[c]
        for k in (2 * x, 2 * x + 1):
            E1[k + 3, pl.ds(8, 16), :] = advance(E, k + 5, k + 3, speed)
    again = boxes(E1, around(3, 2, 2), h2_s, h2_r)

    for way in range(2):
        face_x[way].wait_recv()
    for way in range(2):
        for side, members in enumerate((RISE_X, FALL_X)):
            member = SPEEDS.index((1 - 2 * side, 0, 1 - 2 * way))
            for f, item in enumerate([members.index(member), 5, 6, 7, 8]):
                for h in range(2):
                    both = XR[side, item * 2 + h]
                    DS[way, pl.ds((side * 5 + f) * 2 + h, 1), :] = both[1 - way:2 - way]
    edges = [
        remote(DS.at[0], DR.at[0], pd_s.at[0], pd_r.at[0], place(0, 1)),
        remote(DS.at[1], DR.at[1], pd_s.at[1], pd_r.at[1], place(0, -1)),
    ]
    for copy in edges:
        copy.start()
    for way, (members, row) in enumerate(((RISE_X, 1), (FALL_X, 21))):
        for f, field in enumerate(members + MOMENTS):
            for h in range(2):
                EP[h, field, pl.ds(row, 2), :] = XR[way, f * 2 + h]
    for way, (members, zi) in enumerate(((RISE_Z, 0), (FALL_Z, 3))):
        face_z[way].wait_recv()
        for f, field in enumerate(members + MOMENTS):
            for h in range(2):
                EP[h, field, pl.ds(4 + zi, 4, stride=4), :] = ZR[way, f * 2 + h]
    for way in range(2):
        edges[way].wait_recv()
        for side in range(2):
            row = side * 20 + way * 3
            member = SPEEDS.index((1 - 2 * side, 0, 1 - 2 * way))
            for f, field in enumerate([member] + MOMENTS):
                for h in range(2):
                    EP[h, field, pl.ds(row, 1), :] = DR[way, pl.ds((side * 5 + f) * 2 + h, 1), :]

    wait_all(RF, 5, fs_r)
    half = n // 2
    expand = jnp.where(iota((half, L), 1) // 8 == iota((half, L), 0), 1.0, 0.0).astype(F32)
    for slot in range(5):
        whole = RF[pl.ds(slot, n, stride=8), :]
        for h in range(2):
            q = t_dot(whole[h * half:(h + 1) * half], expand)
            value = q[0:16]
            for y in range(1, 8):
                value = jnp.where(lax.rem(lane, 8) == y, q[y * 16:(y + 1) * 16], value)
            if slot < 4:
                FR[h, pl.ds(slot, 16, stride=4), :] = value
            else:
                FR[h, pl.ds(64, 16), :] = value

    state = []
    for h in range(2):
        mass = EP[h, MASS]
        inverse = 1.0 / mass
        force = [FR[h, pl.ds(c * 24, 24), :] for c in range(3)]
        flow = [(EP[h, MASS + 1 + c] + 0.5 * force[c]) * inverse for c in range(3)]
        square = flow[0] * flow[0] + flow[1] * flow[1] + flow[2] * flow[2]
        work = flow[0] * force[0] + flow[1] * force[1] + flow[2] * force[2]
        state.append((mass, force, flow, 1.0 - 1.5 * square, work))
    rate = 1.0 / RELAX_TIME
    gain = 1.0 - 0.5 / RELAX_TIME

    def along(speed, vector):
        out = None
        for c in range(3):
            if speed[c] == 1:
                out = vector[c] if out is None else out + vector[c]
            elif speed[c] == -1:
                out = -vector[c] if out is None else out - vector[c]
        return out

    for member in range(19):
        cx, cy, cz = SPEEDS[member]
        w = WEIGHTS[member]
        parts = []
        for h in range(2):
            mass, force, flow, rest, work = state[h]
            p = EP[h, member]
            if member == 0:
                new = (rate * w) * mass * rest - (3.0 * gain * w) * work
            else:
                cu, cf = along(SPEEDS[member], flow), along(SPEEDS[member], force)
                new = (rate * w) * mass * (rest + cu * (3.0 + 4.5 * cu)) + (gain * w) * (
                    3.0 * (cf - work) + 9.0 * cu * cf
                )
            parts.append(p * (1.0 - rate) + new)
        if cy:
            turned = [pltpu.roll(v, cy % L, 1) for v in parts]
            edge = lane == (0 if cy == 1 else L - 1)
            parts = [jnp.where(edge, turned[1 - h], turned[h]) for h in range(2)]
        for h in range(2):
            RS[member, h] = parts[h]
            for x in range(4):
                OP[member, x, :, pl.ds(h * L, L)] = RS[
                    member, h, pl.ds((x + 1 - cx) * 4 + 1 - cz, 2), :
                ]

    for copy in again:
        copy.wait_recv()
    potential(E1, 0, 10, 6, 24)
    for x in range(4):
        speed = [SP[c * 4 + x] for c in range(3)]
        for k in (2 * x, 2 * x + 1):
            OD[k] = advance(E1, k + 3, k + 1, speed)

    for copy in halo + again + face_x + face_z + edges:
        copy.wait_send()
    wait_all(SM, 2, ms_s)
    wait_all(SF, 5, fs_s)


def put(dens, pops, dens_out, pops_out, dsem, psem):
    first = pltpu.make_async_copy(dens, dens_out, dsem)
    second = pltpu.make_async_copy(pops, pops_out, psem)
    second.start()
    first.start()
    first.wait()
    second.wait()


def solution(mesh):
    nx, n = mesh.shape["gx"], mesh.shape["gy"]
    L = 4 * n

    def local(density, populations):
        vmem = lambda *shape: pltpu.VMEM(shape, F32)
        dma = lambda *shape: pltpu.SemaphoreType.DMA(shape)
        any_spec = pl.BlockSpec(memory_space=pl.ANY)
        vmem_spec = pl.BlockSpec(memory_space=pltpu.VMEM)
        shapes = (
            jax.ShapeDtypeStruct((8, 16, L), F32),
            jax.ShapeDtypeStruct((19, 4, 2, 2 * L), F32),
        )
        density = pltpu.with_memory_space_constraint(density, pltpu.HBM)
        populations = pltpu.with_memory_space_constraint(populations, pltpu.HBM)
        density, populations = pl.pallas_call(
            lambda *refs: kernel(nx, n, *refs),
            out_shape=shapes,
            in_specs=[any_spec, any_spec],
            out_specs=(vmem_spec, vmem_spec),
            scratch_shapes=[
                vmem(18, 32, L), vmem(14, 32, L), vmem(16, 32, L), vmem(14, 32, L),
                vmem(256, L), vmem(256, L), vmem(12, 16, L),
                vmem(n * 8, 128), vmem(n * 8, 128), vmem(n * 8, 128), vmem(n * 8, 128),
                vmem(256, L), vmem(2, 2, 16, L), vmem(19, 4, 2, 2 * L),
                vmem(2, FIELDS, 24, L), vmem(2, 18, 2, L), vmem(2, 18, 2, L),
                vmem(2, 18, 4, L), vmem(2, 18, 4, L), vmem(2, 24, L), vmem(2, 24, L),
                vmem(2, 80, L), vmem(19, 2, 24, L),
                dma(), dma(),
                dma(8), dma(8), dma(8), dma(8),
                dma(2), dma(2), dma(2), dma(2), dma(2), dma(2),
                dma(), dma(), dma(), dma(),
            ],
            compiler_params=pltpu.CompilerParams(
                collective_id=0, has_side_effects=True, vmem_limit_bytes=16 * 2**20
            ),
        )(density, populations)
        return pl.pallas_call(
            put,
            out_shape=shapes,
            in_specs=[any_spec, any_spec],
            out_specs=(any_spec, any_spec),
            scratch_shapes=[dma(), dma()],
            compiler_params=pltpu.CompilerParams(vmem_limit_bytes=8 * 2**20),
        )(density, populations)

    return jax.shard_map(
        local,
        mesh=mesh,
        in_specs=(P("gx", "gy", None), P(None, "gx", "gy", None)),
        out_specs=(P("gx", "gy", None), P(None, "gx", "gy", None)),
        check_vma=False,
    )
```

```python
import jax
import jax.numpy as jnp
from jax import lax
from jax.experimental import pallas as pl
from jax.experimental.pallas import tpu as pltpu
from jax.sharding import PartitionSpec as P

MESH = pl.DeviceIdType.MESH
EXACT = lax.Precision.HIGHEST
F32 = jnp.float32

TIME_STEP = 0.0008
FORCE_UNIT = 0.005
SPEED_UNIT = 2000.0
RELAX_TIME = 0.8
QUENCH = -0.25

SPEEDS = [
    (0, 0, 0),
    (1, 0, 0), (-1, 0, 0), (0, 1, 0), (0, -1, 0), (0, 0, 1), (0, 0, -1),
    (1, 1, 0), (-1, -1, 0), (1, -1, 0), (-1, 1, 0),
    (1, 0, 1), (-1, 0, -1), (1, 0, -1), (-1, 0, 1),
    (0, 1, 1), (0, -1, -1), (0, 1, -1), (0, -1, 1),
]
WEIGHTS = [1.0 / 3.0] + [1.0 / 18.0] * 6 + [1.0 / 36.0] * 12

MASS = 19
FIELDS = 23
RISE_X = [q for q in range(19) if SPEEDS[q][0] == 1]
FALL_X = [q for q in range(19) if SPEEDS[q][0] == -1]
RISE_Z = [q for q in range(19) if SPEEDS[q][2] == 1]
FALL_Z = [q for q in range(19) if SPEEDS[q][2] == -1]
MOMENTS = [MASS, MASS + 1, MASS + 2, MASS + 3]
DIAGONALS = [(1, 1), (1, -1), (-1, 1), (-1, -1)]


def dot_t(a, b):
    return lax.dot_general(
        a, b, (((1,), (1,)), ((), ())), precision=EXACT, preferred_element_type=F32
    )


def t_dot(a, b):
    return lax.dot_general(
        a, b, (((0,), (0,)), ((), ())), precision=EXACT, preferred_element_type=F32
    )


def iota(shape, dim):
    return lax.broadcasted_iota(jnp.int32, shape, dim)


def kernel(
    nx, n, dens_hbm, pops_hbm, OD, OP,
    E, E1, L1, PT, FA, FB, SP, SF, RF, SM, RM, MQ, MX, PV, EP, XS, XR, ZS, ZR, DS, DR, FR, RS,
    dsem, psem, h1_s, h1_r, h2_s, h2_r, px_s, px_r, pz_s, pz_r, pd_s, pd_r,
    ms_s, ms_r, fs_s, fs_r,
):
    L = 4 * n
    gx = lax.axis_index("gx")
    gy = lax.axis_index("gy")

    def place(sx, sy):
        return {"gx": lax.rem(gx + sx + nx, nx), "gy": lax.rem(gy + sy + n, n)}

    barrier = pltpu.get_barrier_semaphore()
    for sx, sy in ((1, 0), (-1, 0)):
        pl.semaphore_signal(barrier, inc=1, device_id=place(sx, sy), device_id_type=MESH)

    @pl.loop(1, n)
    def _(k):
        pl.semaphore_signal(barrier, inc=1, device_id=place(0, k), device_id_type=MESH)

    dens_in = pltpu.make_async_copy(dens_hbm, E.at[pl.ds(5, 8), pl.ds(8, 16)], dsem)
    dens_in.start()
    pops_in = pltpu.make_async_copy(pops_hbm, PV, psem)
    pops_in.start()

    def remote(src, dst, send, recv, where):
        return pltpu.make_async_remote_copy(
            src_ref=src, dst_ref=dst, send_sem=send, recv_sem=recv, device_id=where,
            device_id_type=MESH,
        )

    lane = iota((1, L), 1)

    pops_in.wait()
    for h in range(2):
        for member in range(19):
            for x in range(4):
                EP[h, member, pl.ds(x * 4 + 5, 2), :] = PV[member, x, :, pl.ds(h * L, L)]
        total = jnp.zeros((24, L), F32)
        moment = [jnp.zeros((24, L), F32) for _ in range(3)]
        for member in range(19):
            value = EP[h, member]
            total = total + value
            for c in range(3):
                if SPEEDS[member][c] == 1:
                    moment[c] = moment[c] + value
                elif SPEEDS[member][c] == -1:
                    moment[c] = moment[c] - value
        EP[h, MASS] = total
        for c in range(3):
            EP[h, MASS + 1 + c] = moment[c]

    for way, (members, row) in enumerate(((RISE_X, 17), (FALL_X, 5))):
        for f, field in enumerate(members + MOMENTS):
            for h in range(2):
                XS[way, f * 2 + h] = EP[h, field, pl.ds(row, 2), :]
    for way, (members, zi) in enumerate(((RISE_Z, 2), (FALL_Z, 1))):
        for f, field in enumerate(members + MOMENTS):
            for h in range(2):
                ZS[way, f * 2 + h] = EP[h, field, pl.ds(4 + zi, 4, stride=4), :]
    spread = [
        jnp.where((iota((n, L), 1) + h * L) // 8 == iota((n, L), 0), 1.0, 0.0).astype(F32)
        for h in range(2)
    ]
    for zl in range(2):
        result = None
        for h in range(2):
            for c in range(4):
                MX[zl, h, pl.ds(c * 4, 4), :] = EP[h, MASS + c, pl.ds(5 + zl, 4, stride=4), :]
            values = MX[zl, h]
            tiles = jnp.concatenate(
                [jnp.where(lax.rem(lane, 8) == y, values, 0.0) for y in range(8)], axis=0
            )
            part = dot_t(spread[h], tiles)
            result = part if result is None else result + part
        SM[pl.ds(zl, n, stride=8), :] = result

    dens_in.wait()
    pl.semaphore_wait(barrier, n + 1)

    def boxes(buf, items, first, send, recv):
        copies = []
        for i, (where, x0, x1, xs, y0, y1, ys) in enumerate(items):
            copies.append(remote(
                buf.at[pl.ds(x0, xs), pl.ds(y0, ys)], buf.at[pl.ds(x1, xs), pl.ds(y1, ys)],
                send.at[first + i], recv.at[first + i], place(*where),
            ))
        for copy in copies:
            copy.start()
        return copies

    def others():
        if n % 32:
            return [lax.rem(gy + k, n) for k in range(1, n)]
        z, inner = gy // 8, lax.rem(gy, 8)
        groups = (3 - z, lax.rem(z + 2, 4), z + 1 - 2 * lax.rem(z, 2), z)
        return [
            to_z * 8 + lax.rem(inner + k, 8)
            for i, to_z in enumerate(groups) for k in range(1 if i == 3 else 0, 8)
        ]

    def to_all(src, dst, rows, send, recv):
        for to in others():
            remote(
                src.at[pl.ds(pl.multiple_of(to * 8, 8), rows)],
                dst.at[pl.ds(pl.multiple_of(gy * 8, 8), rows)],
                send, recv, {"gx": gx, "gy": to},
            ).start()
        for slot in range(rows):
            dst[pl.ds(gy * 8 + slot, 1), :] = src[pl.ds(gy * 8 + slot, 1), :]

    def wait_all(buf, rows, sem):
        whole = buf.at[pl.ds(0, (n - 1) * rows)]
        pltpu.make_async_copy(whole, whole, sem).wait()

    near = boxes(
        E, [((1, 0), 10, 2, 3, 8, 8, 16), ((-1, 0), 5, 13, 3, 8, 8, 16)], 0, h1_s, h1_r
    )
    rows = boxes(
        E, [((0, 1), 5, 5, 8, 21, 5, 3), ((0, -1), 5, 5, 8, 8, 24, 3)], 2, h1_s, h1_r
    )
    far = boxes(
        E, [((1, 0), 8, 0, 2, 8, 8, 16), ((-1, 0), 8, 16, 2, 8, 8, 16)], 4, h1_s, h1_r
    )
    to_all(SM, RM, 2, ms_s, ms_r)
    face_z = [
        remote(ZS.at[0], ZR.at[0], pz_s.at[0], pz_r.at[0], place(0, 1)),
        remote(ZS.at[1], ZR.at[1], pz_s.at[1], pz_r.at[1], place(0, -1)),
    ]
    face_x = [
        remote(XS.at[0], XR.at[0], px_s.at[0], px_r.at[0], place(1, 0)),
        remote(XS.at[1], XR.at[1], px_s.at[1], px_r.at[1], place(-1, 0)),
    ]
    for copy in face_z + face_x:
        copy.start()

    for copy in rows:
        copy.wait_recv()
    corners = boxes(
        E,
        [
            (where, x0, x1, 4, y0, y0, 3)
            for where, x0, x1 in (((1, 0), 9, 1), ((-1, 0), 5, 13)) for y0 in (5, 24)
        ],
        6, h1_s, h1_r,
    )
    for way in range(2):
        face_z[way].wait_recv()
    for way, (sx, x) in enumerate(((1, 3), (-1, 0))):
        for side, members in enumerate((RISE_Z, FALL_Z)):
            member = SPEEDS.index((sx, 0, 1 - 2 * side))
            for f, item in enumerate([members.index(member), 5, 6, 7, 8]):
                for h in range(2):
                    DS[way, pl.ds((side * 5 + f) * 2 + h, 1), :] = ZR[
                        side, item * 2 + h, pl.ds(x, 1), :
                    ]
    edges = [
        remote(DS.at[0], DR.at[0], pd_s.at[0], pd_r.at[0], place(1, 0)),
        remote(DS.at[1], DR.at[1], pd_s.at[1], pd_r.at[1], place(-1, 0)),
    ]
    for copy in edges:
        copy.start()
    for way, (members, zi) in enumerate(((RISE_Z, 0), (FALL_Z, 3))):
        for f, field in enumerate(members + MOMENTS):
            for h in range(2):
                EP[h, field, pl.ds(4 + zi, 4, stride=4), :] = ZR[way, f * 2 + h]

    def turn(value, by):
        return pltpu.roll(value, by % L, 1)

    def lap(ref, i, r0, rows):
        c = ref[i, pl.ds(r0, rows), :]
        return c, (
            -6.0 * c + ref[i - 1, pl.ds(r0, rows), :] + ref[i + 1, pl.ds(r0, rows), :]
            + ref[i, pl.ds(r0 - 1, rows), :] + ref[i, pl.ds(r0 + 1, rows), :]
            + turn(c, 1) + turn(c, -1)
        )

    def potential(src, outer, inner, r0, rows):
        for i in outer:
            L1[i, pl.ds(0, rows), :] = lap(src, i + 1, r0, rows)[1]
        for j in inner:
            c, second = lap(L1, j + 1, 1, rows)
            rho = src[j + 2, pl.ds(r0 + 1, rows), :]
            PT[j, pl.ds(0, rows), :] = (
                (QUENCH + 1.0) * rho + 2.0 * c + second + rho * rho * rho
            )

    wait_all(RM, 2, ms_r)
    shape = (2 * n, L)
    row = iota(shape, 0)
    pick = iota(shape, 1) // 2 == 2 * lax.rem(row, n) + row // n
    both = jnp.concatenate([RM[pl.ds(zl, n, stride=8), :] for zl in range(2)], axis=0)
    wide = t_dot(both, jnp.where(pick, 1.0, 0.0).astype(F32))
    for y in range(16):
        MQ[pl.ds(y * 16, 16), :] = wide[(y // 2) * 16:(y // 2 + 1) * 16]

    for copy in near + corners:
        copy.wait_recv()
    potential(E, range(2, 14), range(2, 12), 6, 24)

    scale = -0.5 * FORCE_UNIT * 0.125
    zeros = jnp.zeros((16, L), F32)
    for extra in range(8, 16):
        FB[pl.ds(extra, 16, stride=16), :] = zeros

    def force_pair(src, e0, p0, r0, rows):
        sums = [None, None, None]
        for k in range(2):
            rho = src[e0 + k, pl.ds(r0, rows), :] * scale
            mid = PT[p0 + k, pl.ds(1, rows), :]
            parts = (
                PT[p0 + k + 1, pl.ds(1, rows), :] - PT[p0 + k - 1, pl.ds(1, rows), :],
                PT[p0 + k, pl.ds(2, rows), :] - PT[p0 + k, pl.ds(0, rows), :],
                turn(mid, -1) - turn(mid, 1),
            )
            for c in range(3):
                value = rho * parts[c]
                sums[c] = value if sums[c] is None else sums[c] + value
        return sums

    def outgoing(xi):
        sums = force_pair(E, 2 * xi + 3, 2 * xi + 1, 8, 16)
        for c in range(3):
            cx = c * 6 + xi
            if 1 <= xi <= 4:
                SP[c * 4 + xi - 1] = sums[c]
            if cx < 16:
                FA[pl.ds(cx, 16, stride=16), :] = sums[c]
            else:
                for zl in range(4):
                    FB[pl.ds((cx - 16) * 4 + zl, 16, stride=16), :] = turn(
                        sums[c], -2 * (zl - 1)
                    )

    for xi in range(1, 5):
        outgoing(xi)

    even_y = lax.rem(iota((16, L), 0), 2) == 0
    even_z = lax.rem(iota((16, L), 1), 2) == 0

    def fine_speed(x):
        mass = MQ[pl.ds(x, 16, stride=16), :]
        inverse = SPEED_UNIT * 0.5 / mass
        out = []
        for c in range(3):
            s = SP[c * 4 + x]
            s = s + jnp.where(even_y, pltpu.roll(s, 15, 0), pltpu.roll(s, 1, 0))
            s = s + jnp.where(even_z, turn(s, -1), turn(s, 1))
            m = MQ[pl.ds((c + 1) * 4 + x, 16, stride=16), :]
            out.append((m + 0.5 * s) * inverse)
        return out

    def advance(src, e, p, speed):
        mid = src[e, pl.ds(8, 16), :]
        advect = (
            speed[0] * (src[e + 1, pl.ds(8, 16), :] - src[e - 1, pl.ds(8, 16), :])
            + speed[1] * (src[e, pl.ds(9, 16), :] - src[e, pl.ds(7, 16), :])
            + speed[2] * (turn(mid, -1) - turn(mid, 1))
        )
        return mid + TIME_STEP * (lap(PT, p, 1, 16)[1] - advect)

    for x in range(4):
        speed = fine_speed(x)
        for c in range(3):
            SP[c * 4 + x] = speed[c]
        for k in (2 * x, 2 * x + 1):
            E1[k + 3, pl.ds(8, 16), :] = advance(E, k + 5, k + 3, speed)
    again = boxes(
        E1,
        [
            ((sx, sy), *((9, 1, 2) if sx == 1 else (3, 11, 2)),
             *((22, 6, 2) if sy == 1 else (8, 24, 2)))
            for sx, sy in DIAGONALS
        ] + [
            ((1, 0), 8, 0, 3, 8, 8, 16),
            ((-1, 0), 3, 11, 3, 8, 8, 16),
            ((0, 1), 3, 3, 8, 21, 5, 3),
            ((0, -1), 3, 3, 8, 8, 24, 3),
        ],
        0, h2_s, h2_r,
    )

    for copy in far:
        copy.wait_recv()
    potential(E, (0, 1, 14, 15), (0, 1, 12, 13), 6, 24)
    for xi in (0, 5):
        outgoing(xi)

    shape = (4 * n, L)
    row = iota(shape, 0)
    window = lax.rem(2 * lax.rem(row, n) - 1 + row // n + 2 * n, 2 * n)
    choose = jnp.where(iota(shape, 1) // 2 == window, 1.0, 0.0).astype(F32)
    ga = jnp.concatenate(
        [FA[pl.ds(32 * y, 16), :] + FA[pl.ds(32 * y + 16, 16), :] for y in range(8)], axis=0
    )
    gb = jnp.concatenate(
        [FB[pl.ds(32 * y, 16), :] + FB[pl.ds(32 * y + 16, 16), :] for y in range(8)], axis=0
    )
    ta = dot_t(choose, ga)
    tb = dot_t(choose[n:2 * n], gb)
    for zl in range(4):
        SF[pl.ds(zl, n, stride=8), :] = ta[zl * n:(zl + 1) * n]
    SF[pl.ds(4, n, stride=8), :] = tb

    to_all(SF, RF, 5, fs_s, fs_r)

    for way in range(2):
        face_x[way].wait_recv()
    for way, (members, row) in enumerate(((RISE_X, 1), (FALL_X, 21))):
        for f, field in enumerate(members + MOMENTS):
            for h in range(2):
                EP[h, field, pl.ds(row, 2), :] = XR[way, f * 2 + h]
    for way in range(2):
        edges[way].wait_recv()
        for side, members in enumerate((RISE_Z, FALL_Z)):
            member = SPEEDS.index((1 - 2 * way, 0, 1 - 2 * side))
            row = way * 20 + side * 3
            for f, field in enumerate([member] + MOMENTS):
                for h in range(2):
                    EP[h, field, pl.ds(row, 1), :] = DR[way, pl.ds((side * 5 + f) * 2 + h, 1), :]

    wait_all(RF, 5, fs_r)
    half = n // 2
    expand = jnp.where(iota((half, L), 1) // 8 == iota((half, L), 0), 1.0, 0.0).astype(F32)
    for slot in range(5):
        whole = RF[pl.ds(slot, n, stride=8), :]
        for h in range(2):
            q = t_dot(whole[h * half:(h + 1) * half], expand)
            value = q[0:16]
            for y in range(1, 8):
                value = jnp.where(lax.rem(lane, 8) == y, q[y * 16:(y + 1) * 16], value)
            if slot < 4:
                FR[h, pl.ds(slot, 16, stride=4), :] = value
            else:
                FR[h, pl.ds(64, 16), :] = value

    state = []
    for h in range(2):
        mass = EP[h, MASS]
        inverse = 1.0 / mass
        force = [FR[h, pl.ds(c * 24, 24), :] for c in range(3)]
        flow = [(EP[h, MASS + 1 + c] + 0.5 * force[c]) * inverse for c in range(3)]
        square = flow[0] * flow[0] + flow[1] * flow[1] + flow[2] * flow[2]
        work = flow[0] * force[0] + flow[1] * force[1] + flow[2] * force[2]
        state.append((mass, force, flow, 1.0 - 1.5 * square, work))
    rate = 1.0 / RELAX_TIME
    gain = 1.0 - 0.5 / RELAX_TIME

    def along(speed, vector):
        out = None
        for c in range(3):
            if speed[c] == 1:
                out = vector[c] if out is None else out + vector[c]
            elif speed[c] == -1:
                out = -vector[c] if out is None else out - vector[c]
        return out

    for member in range(19):
        cx, cy, cz = SPEEDS[member]
        w = WEIGHTS[member]
        parts = []
        for h in range(2):
            mass, force, flow, rest, work = state[h]
            p = EP[h, member]
            if member == 0:
                new = (rate * w) * mass * rest - (3.0 * gain * w) * work
            else:
                cu, cf = along(SPEEDS[member], flow), along(SPEEDS[member], force)
                new = (rate * w) * mass * (rest + cu * (3.0 + 4.5 * cu)) + (gain * w) * (
                    3.0 * (cf - work) + 9.0 * cu * cf
                )
            parts.append(p * (1.0 - rate) + new)
        if cy:
            turned = [pltpu.roll(v, cy % L, 1) for v in parts]
            edge = lane == (0 if cy == 1 else L - 1)
            parts = [jnp.where(edge, turned[1 - h], turned[h]) for h in range(2)]
        for h in range(2):
            RS[member, h] = parts[h]
            for x in range(4):
                OP[member, x, :, pl.ds(h * L, L)] = RS[
                    member, h, pl.ds((x + 1 - cx) * 4 + 1 - cz, 2), :
                ]

    for copy in again:
        copy.wait_recv()
    potential(E1, range(12), range(10), 6, 24)
    for x in range(4):
        speed = [SP[c * 4 + x] for c in range(3)]
        for k in (2 * x, 2 * x + 1):
            OD[k] = advance(E1, k + 3, k + 1, speed)

    for copy in near + rows + far + corners + again + face_x + face_z + edges:
        copy.wait_send()
    wait_all(SM, 2, ms_s)
    wait_all(SF, 5, fs_s)


def put(dens, pops, dens_out, pops_out, dsem, psem):
    first = pltpu.make_async_copy(dens, dens_out, dsem)
    second = pltpu.make_async_copy(pops, pops_out, psem)
    second.start()
    first.start()
    first.wait()
    second.wait()


def solution(mesh):
    nx, n = mesh.shape["gx"], mesh.shape["gy"]
    L = 4 * n

    def local(density, populations):
        vmem = lambda *shape: pltpu.VMEM(shape, F32)
        dma = lambda *shape: pltpu.SemaphoreType.DMA(shape)
        any_spec = pl.BlockSpec(memory_space=pl.ANY)
        vmem_spec = pl.BlockSpec(memory_space=pltpu.VMEM)
        shapes = (
            jax.ShapeDtypeStruct((8, 16, L), F32),
            jax.ShapeDtypeStruct((19, 4, 2, 2 * L), F32),
        )
        density = pltpu.with_memory_space_constraint(density, pltpu.HBM)
        populations = pltpu.with_memory_space_constraint(populations, pltpu.HBM)
        density, populations = pl.pallas_call(
            lambda *refs: kernel(nx, n, *refs),
            out_shape=shapes,
            in_specs=[any_spec, any_spec],
            out_specs=(vmem_spec, vmem_spec),
            scratch_shapes=[
                vmem(18, 32, L), vmem(14, 32, L), vmem(16, 32, L), vmem(14, 32, L),
                vmem(256, L), vmem(256, L), vmem(12, 16, L),
                vmem(n * 8, 128), vmem(n * 8, 128), vmem(n * 8, 128), vmem(n * 8, 128),
                vmem(256, L), vmem(2, 2, 16, L), vmem(19, 4, 2, 2 * L),
                vmem(2, FIELDS, 24, L), vmem(2, 18, 2, L), vmem(2, 18, 2, L),
                vmem(2, 18, 4, L), vmem(2, 18, 4, L), vmem(2, 20, L), vmem(2, 20, L),
                vmem(2, 80, L), vmem(19, 2, 24, L),
                dma(), dma(),
                dma(10), dma(10), dma(8), dma(8),
                dma(2), dma(2), dma(2), dma(2), dma(2), dma(2),
                dma(), dma(), dma(), dma(),
            ],
            compiler_params=pltpu.CompilerParams(
                collective_id=0, has_side_effects=True, vmem_limit_bytes=16 * 2**20
            ),
        )(density, populations)
        return pl.pallas_call(
            put,
            out_shape=shapes,
            in_specs=[any_spec, any_spec],
            out_specs=(any_spec, any_spec),
            scratch_shapes=[dma(), dma()],
            compiler_params=pltpu.CompilerParams(vmem_limit_bytes=8 * 2**20),
        )(density, populations)

    return jax.shard_map(
        local,
        mesh=mesh,
        in_specs=(P("gx", "gy", None), P(None, "gx", "gy", None)),
        out_specs=(P("gx", "gy", None), P(None, "gx", "gy", None)),
        check_vma=False,
    )
```

```python
import jax
import jax.numpy as jnp
from jax import lax
from jax.experimental import pallas as pl
from jax.experimental.pallas import tpu as pltpu
from jax.sharding import PartitionSpec as P

MESH = pl.DeviceIdType.MESH
EXACT = lax.Precision.HIGHEST
F32 = jnp.float32

TIME_STEP = 0.0008
FORCE_UNIT = 0.005
SPEED_UNIT = 2000.0
RELAX_TIME = 0.8
QUENCH = -0.25

SPEEDS = [
    (0, 0, 0),
    (1, 0, 0), (-1, 0, 0), (0, 1, 0), (0, -1, 0), (0, 0, 1), (0, 0, -1),
    (1, 1, 0), (-1, -1, 0), (1, -1, 0), (-1, 1, 0),
    (1, 0, 1), (-1, 0, -1), (1, 0, -1), (-1, 0, 1),
    (0, 1, 1), (0, -1, -1), (0, 1, -1), (0, -1, 1),
]
WEIGHTS = [1.0 / 3.0] + [1.0 / 18.0] * 6 + [1.0 / 36.0] * 12

MASS = 19
FIELDS = 23
RISE_X = [q for q in range(19) if SPEEDS[q][0] == 1]
FALL_X = [q for q in range(19) if SPEEDS[q][0] == -1]
RISE_Z = [q for q in range(19) if SPEEDS[q][2] == 1]
FALL_Z = [q for q in range(19) if SPEEDS[q][2] == -1]
MOMENTS = [MASS, MASS + 1, MASS + 2, MASS + 3]
DIAGONALS = [(1, 1), (1, -1), (-1, 1), (-1, -1)]


def dot_t(a, b):
    return lax.dot_general(
        a, b, (((1,), (1,)), ((), ())), precision=EXACT, preferred_element_type=F32
    )


def t_dot(a, b):
    return lax.dot_general(
        a, b, (((0,), (0,)), ((), ())), precision=EXACT, preferred_element_type=F32
    )


def iota(shape, dim):
    return lax.broadcasted_iota(jnp.int32, shape, dim)


def kernel(
    nx, n, dens_hbm, pops_hbm, OD, OP,
    E, E1, L1, PT, FA, FB, SP, SF, RF, SM, RM, MQ, MX, PV, EP, XS, XR, ZS, ZR, DS, DR, FR, RS,
    dsem, psem, h1_s, h1_r, h2_s, h2_r, px_s, px_r, pz_s, pz_r, pd_s, pd_r,
    ms_s, ms_r, fs_s, fs_r,
):
    L = 4 * n
    gx = lax.axis_index("gx")
    gy = lax.axis_index("gy")

    def place(sx, sy):
        return {"gx": lax.rem(gx + sx + nx, nx), "gy": lax.rem(gy + sy + n, n)}

    barrier = pltpu.get_barrier_semaphore()
    for sx, sy in ((1, 0), (-1, 0)):
        pl.semaphore_signal(barrier, inc=1, device_id=place(sx, sy), device_id_type=MESH)

    @pl.loop(1, n)
    def _(k):
        pl.semaphore_signal(barrier, inc=1, device_id=place(0, k), device_id_type=MESH)

    dens_in = pltpu.make_async_copy(dens_hbm, E.at[pl.ds(5, 8), pl.ds(8, 16)], dsem)
    dens_in.start()
    pops_in = pltpu.make_async_copy(pops_hbm, PV, psem)
    pops_in.start()

    def remote(src, dst, send, recv, where):
        return pltpu.make_async_remote_copy(
            src_ref=src, dst_ref=dst, send_sem=send, recv_sem=recv, device_id=where,
            device_id_type=MESH,
        )

    lane = iota((1, L), 1)

    pops_in.wait()
    for h in range(2):
        for member in range(19):
            for x in range(4):
                EP[h, member, pl.ds(x * 4 + 5, 2), :] = PV[member, x, :, pl.ds(h * L, L)]
        total = jnp.zeros((24, L), F32)
        moment = [jnp.zeros((24, L), F32) for _ in range(3)]
        for member in range(19):
            value = EP[h, member]
            total = total + value
            for c in range(3):
                if SPEEDS[member][c] == 1:
                    moment[c] = moment[c] + value
                elif SPEEDS[member][c] == -1:
                    moment[c] = moment[c] - value
        EP[h, MASS] = total
        for c in range(3):
            EP[h, MASS + 1 + c] = moment[c]

    for way, (members, row) in enumerate(((RISE_X, 17), (FALL_X, 5))):
        for f, field in enumerate(members + MOMENTS):
            for h in range(2):
                XS[way, f * 2 + h] = EP[h, field, pl.ds(row, 2), :]
    for way, (members, zi) in enumerate(((RISE_Z, 2), (FALL_Z, 1))):
        for f, field in enumerate(members + MOMENTS):
            for h in range(2):
                ZS[way, f * 2 + h] = EP[h, field, pl.ds(4 + zi, 4, stride=4), :]
    spread = [
        jnp.where((iota((n, L), 1) + h * L) // 8 == iota((n, L), 0), 1.0, 0.0).astype(F32)
        for h in range(2)
    ]
    for zl in range(2):
        result = None
        for h in range(2):
            for c in range(4):
                MX[zl, h, pl.ds(c * 4, 4), :] = EP[h, MASS + c, pl.ds(5 + zl, 4, stride=4), :]
            values = MX[zl, h]
            tiles = jnp.concatenate(
                [jnp.where(lax.rem(lane, 8) == y, values, 0.0) for y in range(8)], axis=0
            )
            part = dot_t(spread[h], tiles)
            result = part if result is None else result + part
        SM[pl.ds(zl, n, stride=8), :] = result

    dens_in.wait()
    pl.semaphore_wait(barrier, n + 1)

    def boxes(buf, items, first, send, recv):
        copies = []
        for i, (where, x0, x1, xs, y0, y1, ys) in enumerate(items):
            copies.append(remote(
                buf.at[pl.ds(x0, xs), pl.ds(y0, ys)], buf.at[pl.ds(x1, xs), pl.ds(y1, ys)],
                send.at[first + i], recv.at[first + i], place(*where),
            ))
        for copy in copies:
            copy.start()
        return copies

    def others():
        if n % 32:
            return [lax.rem(gy + k, n) for k in range(1, n)]
        z, inner = gy // 8, lax.rem(gy, 8)
        groups = (3 - z, lax.rem(z + 2, 4), z + 1 - 2 * lax.rem(z, 2), z)
        return [
            to_z * 8 + lax.rem(inner + k, 8)
            for i, to_z in enumerate(groups) for k in range(1 if i == 3 else 0, 8)
        ]

    def to_all(src, dst, rows, send, recv):
        for to in others():
            remote(
                src.at[pl.ds(pl.multiple_of(to * 8, 8), rows)],
                dst.at[pl.ds(pl.multiple_of(gy * 8, 8), rows)],
                send, recv, {"gx": gx, "gy": to},
            ).start()
        for slot in range(rows):
            dst[pl.ds(gy * 8 + slot, 1), :] = src[pl.ds(gy * 8 + slot, 1), :]

    def wait_all(buf, rows, sem):
        whole = buf.at[pl.ds(0, (n - 1) * rows)]
        pltpu.make_async_copy(whole, whole, sem).wait()

    near = boxes(
        E, [((1, 0), 10, 2, 3, 8, 8, 16), ((-1, 0), 5, 13, 3, 8, 8, 16)], 0, h1_s, h1_r
    )
    rows = boxes(
        E, [((0, 1), 5, 5, 8, 21, 5, 3), ((0, -1), 5, 5, 8, 8, 24, 3)], 2, h1_s, h1_r
    )
    far = boxes(
        E, [((1, 0), 8, 0, 2, 8, 8, 16), ((-1, 0), 8, 16, 2, 8, 8, 16)], 4, h1_s, h1_r
    )
    to_all(SM, RM, 2, ms_s, ms_r)
    face_z = [
        remote(ZS.at[0], ZR.at[0], pz_s.at[0], pz_r.at[0], place(0, 1)),
        remote(ZS.at[1], ZR.at[1], pz_s.at[1], pz_r.at[1], place(0, -1)),
    ]
    face_x = [
        remote(XS.at[0], XR.at[0], px_s.at[0], px_r.at[0], place(1, 0)),
        remote(XS.at[1], XR.at[1], px_s.at[1], px_r.at[1], place(-1, 0)),
    ]
    for copy in face_z + face_x:
        copy.start()

    for copy in rows:
        copy.wait_recv()
    corners = boxes(
        E,
        [
            (where, x0, x1, 4, y0, y0, 3)
            for where, x0, x1 in (((1, 0), 9, 1), ((-1, 0), 5, 13)) for y0 in (5, 24)
        ],
        6, h1_s, h1_r,
    )
    for way in range(2):
        face_z[way].wait_recv()
    for way, (sx, x) in enumerate(((1, 3), (-1, 0))):
        for side, members in enumerate((RISE_Z, FALL_Z)):
            member = SPEEDS.index((sx, 0, 1 - 2 * side))
            for f, item in enumerate([members.index(member), 5, 6, 7, 8]):
                for h in range(2):
                    DS[way, pl.ds((side * 5 + f) * 2 + h, 1), :] = ZR[
                        side, item * 2 + h, pl.ds(x, 1), :
                    ]
    edges = [
        remote(DS.at[0], DR.at[0], pd_s.at[0], pd_r.at[0], place(1, 0)),
        remote(DS.at[1], DR.at[1], pd_s.at[1], pd_r.at[1], place(-1, 0)),
    ]
    for copy in edges:
        copy.start()
    for way, (members, zi) in enumerate(((RISE_Z, 0), (FALL_Z, 3))):
        for f, field in enumerate(members + MOMENTS):
            for h in range(2):
                EP[h, field, pl.ds(4 + zi, 4, stride=4), :] = ZR[way, f * 2 + h]

    def turn(value, by):
        return pltpu.roll(value, by % L, 1)

    def lap(ref, i, r0, rows):
        c = ref[i, pl.ds(r0, rows), :]
        return c, (
            -6.0 * c + ref[i - 1, pl.ds(r0, rows), :] + ref[i + 1, pl.ds(r0, rows), :]
            + ref[i, pl.ds(r0 - 1, rows), :] + ref[i, pl.ds(r0 + 1, rows), :]
            + turn(c, 1) + turn(c, -1)
        )

    def potential(src, outer, inner, r0, rows):
        for i in outer:
            L1[i, pl.ds(0, rows), :] = lap(src, i + 1, r0, rows)[1]
        for j in inner:
            c, second = lap(L1, j + 1, 1, rows)
            rho = src[j + 2, pl.ds(r0 + 1, rows), :]
            PT[j, pl.ds(0, rows), :] = (
                (QUENCH + 1.0) * rho + 2.0 * c + second + rho * rho * rho
            )

    wait_all(RM, 2, ms_r)
    shape = (2 * n, L)
    row = iota(shape, 0)
    pick = iota(shape, 1) // 2 == 2 * lax.rem(row, n) + row // n
    both = jnp.concatenate([RM[pl.ds(zl, n, stride=8), :] for zl in range(2)], axis=0)
    wide = t_dot(both, jnp.where(pick, 1.0, 0.0).astype(F32))
    for y in range(16):
        MQ[pl.ds(y * 16, 16), :] = wide[(y // 2) * 16:(y // 2 + 1) * 16]

    potential(E, range(5, 11), range(5, 9), 6, 24)
    for copy in near + corners:
        copy.wait_recv()
    potential(E, (2, 3, 4, 11, 12, 13), (2, 3, 4, 9, 10, 11), 6, 24)

    scale = -0.5 * FORCE_UNIT * 0.125
    zeros = jnp.zeros((16, L), F32)
    for extra in range(8, 16):
        FB[pl.ds(extra, 16, stride=16), :] = zeros

    def force_pair(src, e0, p0, r0, rows):
        sums = [None, None, None]
        for k in range(2):
            rho = src[e0 + k, pl.ds(r0, rows), :] * scale
            mid = PT[p0 + k, pl.ds(1, rows), :]
            parts = (
                PT[p0 + k + 1, pl.ds(1, rows), :] - PT[p0 + k - 1, pl.ds(1, rows), :],
                PT[p0 + k, pl.ds(2, rows), :] - PT[p0 + k, pl.ds(0, rows), :],
                turn(mid, -1) - turn(mid, 1),
            )
            for c in range(3):
                value = rho * parts[c]
                sums[c] = value if sums[c] is None else sums[c] + value
        return sums

    def outgoing(xi):
        sums = force_pair(E, 2 * xi + 3, 2 * xi + 1, 8, 16)
        for c in range(3):
            cx = c * 6 + xi
            if 1 <= xi <= 4:
                SP[c * 4 + xi - 1] = sums[c]
            if cx < 16:
                FA[pl.ds(cx, 16, stride=16), :] = sums[c]
            else:
                for zl in range(4):
                    FB[pl.ds((cx - 16) * 4 + zl, 16, stride=16), :] = turn(
                        sums[c], -2 * (zl - 1)
                    )

    for xi in range(1, 5):
        outgoing(xi)

    even_y = lax.rem(iota((16, L), 0), 2) == 0
    even_z = lax.rem(iota((16, L), 1), 2) == 0

    def fine_speed(x):
        mass = MQ[pl.ds(x, 16, stride=16), :]
        inverse = SPEED_UNIT * 0.5 / mass
        out = []
        for c in range(3):
            s = SP[c * 4 + x]
            s = s + jnp.where(even_y, pltpu.roll(s, 15, 0), pltpu.roll(s, 1, 0))
            s = s + jnp.where(even_z, turn(s, -1), turn(s, 1))
            m = MQ[pl.ds((c + 1) * 4 + x, 16, stride=16), :]
            out.append((m + 0.5 * s) * inverse)
        return out

    def advance(src, e, p, speed):
        mid = src[e, pl.ds(8, 16), :]
        advect = (
            speed[0] * (src[e + 1, pl.ds(8, 16), :] - src[e - 1, pl.ds(8, 16), :])
            + speed[1] * (src[e, pl.ds(9, 16), :] - src[e, pl.ds(7, 16), :])
            + speed[2] * (turn(mid, -1) - turn(mid, 1))
        )
        return mid + TIME_STEP * (lap(PT, p, 1, 16)[1] - advect)

    for x in range(4):
        speed = fine_speed(x)
        for c in range(3):
            SP[c * 4 + x] = speed[c]
        for k in (2 * x, 2 * x + 1):
            E1[k + 3, pl.ds(8, 16), :] = advance(E, k + 5, k + 3, speed)
    again = boxes(
        E1,
        [
            ((sx, sy), *((9, 1, 2) if sx == 1 else (3, 11, 2)),
             *((22, 6, 2) if sy == 1 else (8, 24, 2)))
            for sx, sy in DIAGONALS
        ] + [
            ((1, 0), 8, 0, 3, 8, 8, 16),
            ((-1, 0), 3, 11, 3, 8, 8, 16),
            ((0, 1), 3, 3, 8, 21, 5, 3),
            ((0, -1), 3, 3, 8, 8, 24, 3),
        ],
        0, h2_s, h2_r,
    )

    for copy in far:
        copy.wait_recv()
    potential(E, (0, 1, 14, 15), (0, 1, 12, 13), 6, 24)
    for xi in (0, 5):
        outgoing(xi)

    shape = (4 * n, L)
    row = iota(shape, 0)
    window = lax.rem(2 * lax.rem(row, n) - 1 + row // n + 2 * n, 2 * n)
    choose = jnp.where(iota(shape, 1) // 2 == window, 1.0, 0.0).astype(F32)
    ga = jnp.concatenate(
        [FA[pl.ds(32 * y, 16), :] + FA[pl.ds(32 * y + 16, 16), :] for y in range(8)], axis=0
    )
    gb = jnp.concatenate(
        [FB[pl.ds(32 * y, 16), :] + FB[pl.ds(32 * y + 16, 16), :] for y in range(8)], axis=0
    )
    ta = dot_t(choose, ga)
    tb = dot_t(choose[n:2 * n], gb)
    for zl in range(4):
        SF[pl.ds(zl, n, stride=8), :] = ta[zl * n:(zl + 1) * n]
    SF[pl.ds(4, n, stride=8), :] = tb

    to_all(SF, RF, 5, fs_s, fs_r)

    for way in range(2):
        face_x[way].wait_recv()
    for way, (members, row) in enumerate(((RISE_X, 1), (FALL_X, 21))):
        for f, field in enumerate(members + MOMENTS):
            for h in range(2):
                EP[h, field, pl.ds(row, 2), :] = XR[way, f * 2 + h]
    for way in range(2):
        edges[way].wait_recv()
        for side, members in enumerate((RISE_Z, FALL_Z)):
            member = SPEEDS.index((1 - 2 * way, 0, 1 - 2 * side))
            row = way * 20 + side * 3
            for f, field in enumerate([member] + MOMENTS):
                for h in range(2):
                    EP[h, field, pl.ds(row, 1), :] = DR[way, pl.ds((side * 5 + f) * 2 + h, 1), :]

    for copy in again:
        copy.wait_recv()
    potential(E1, range(12), range(10), 6, 24)
    for x in range(4):
        speed = [SP[c * 4 + x] for c in range(3)]
        for k in (2 * x, 2 * x + 1):
            OD[k] = advance(E1, k + 3, k + 1, speed)

    wait_all(RF, 5, fs_r)
    half = n // 2
    expand = jnp.where(iota((half, L), 1) // 8 == iota((half, L), 0), 1.0, 0.0).astype(F32)
    for slot in range(5):
        whole = RF[pl.ds(slot, n, stride=8), :]
        for h in range(2):
            q = t_dot(whole[h * half:(h + 1) * half], expand)
            value = q[0:16]
            for y in range(1, 8):
                value = jnp.where(lax.rem(lane, 8) == y, q[y * 16:(y + 1) * 16], value)
            if slot < 4:
                FR[h, pl.ds(slot, 16, stride=4), :] = value
            else:
                FR[h, pl.ds(64, 16), :] = value

    rate = 1.0 / RELAX_TIME
    gain = 1.0 - 0.5 / RELAX_TIME
    state = []
    for h in range(2):
        mass = EP[h, MASS]
        inverse = 1.0 / mass
        force = [FR[h, pl.ds(c * 24, 24), :] for c in range(3)]
        flow = [(EP[h, MASS + 1 + c] + 0.5 * force[c]) * inverse for c in range(3)]
        square = flow[0] * flow[0] + flow[1] * flow[1] + flow[2] * flow[2]
        work = flow[0] * force[0] + flow[1] * force[1] + flow[2] * force[2]
        common = rate * mass * (1.0 - 1.5 * square) - (3.0 * gain) * work
        state.append((3.0 * rate * mass, force, flow, common))

    def along(speed, vector):
        out = None
        for c in range(3):
            if speed[c] == 1:
                out = vector[c] if out is None else out + vector[c]
            elif speed[c] == -1:
                out = -vector[c] if out is None else out - vector[c]
        return out

    def passed(member, parts):
        cx, cy, cz = SPEEDS[member]
        parts = [EP[h, member] * (1.0 - rate) + parts[h] for h in range(2)]
        if cy:
            turned = [pltpu.roll(v, cy % L, 1) for v in parts]
            edge = lane == (0 if cy == 1 else L - 1)
            parts = [jnp.where(edge, turned[1 - h], turned[h]) for h in range(2)]
        for h in range(2):
            RS[member, h] = parts[h]
            for x in range(4):
                OP[member, x, :, pl.ds(h * L, L)] = RS[
                    member, h, pl.ds((x + 1 - cx) * 4 + 1 - cz, 2), :
                ]

    passed(0, [WEIGHTS[0] * state[h][3] for h in range(2)])
    scaled = {}
    for w in (WEIGHTS[1], WEIGHTS[7]):
        scaled[w] = [(w * state[h][0], w * state[h][3]) for h in range(2)]
    for member in range(1, 19, 2):
        w = WEIGHTS[member]
        plus, minus = [], []
        for h in range(2):
            mass, common = scaled[w][h]
            cu, cf = along(SPEEDS[member], state[h][2]), along(SPEEDS[member], state[h][1])
            first, second = mass * cu, (3.0 * gain * w) * cf
            odd = first + second
            even = common + cu * (1.5 * first + 3.0 * second)
            plus.append(even + odd)
            minus.append(even - odd)
        passed(member, plus)
        passed(member + 1, minus)

    for copy in near + rows + far + corners + again + face_x + face_z + edges:
        copy.wait_send()
    wait_all(SM, 2, ms_s)
    wait_all(SF, 5, fs_s)


def put(dens, pops, dens_out, pops_out, dsem, psem):
    first = pltpu.make_async_copy(dens, dens_out, dsem)
    second = pltpu.make_async_copy(pops, pops_out, psem)
    second.start()
    first.start()
    first.wait()
    second.wait()


def solution(mesh):
    nx, n = mesh.shape["gx"], mesh.shape["gy"]
    L = 4 * n

    def local(density, populations):
        vmem = lambda *shape: pltpu.VMEM(shape, F32)
        dma = lambda *shape: pltpu.SemaphoreType.DMA(shape)
        any_spec = pl.BlockSpec(memory_space=pl.ANY)
        vmem_spec = pl.BlockSpec(memory_space=pltpu.VMEM)
        shapes = (
            jax.ShapeDtypeStruct((8, 16, L), F32),
            jax.ShapeDtypeStruct((19, 4, 2, 2 * L), F32),
        )
        density = pltpu.with_memory_space_constraint(density, pltpu.HBM)
        populations = pltpu.with_memory_space_constraint(populations, pltpu.HBM)
        density, populations = pl.pallas_call(
            lambda *refs: kernel(nx, n, *refs),
            out_shape=shapes,
            in_specs=[any_spec, any_spec],
            out_specs=(vmem_spec, vmem_spec),
            scratch_shapes=[
                vmem(18, 32, L), vmem(14, 32, L), vmem(16, 32, L), vmem(14, 32, L),
                vmem(256, L), vmem(256, L), vmem(12, 16, L),
                vmem(n * 8, 128), vmem(n * 8, 128), vmem(n * 8, 128), vmem(n * 8, 128),
                vmem(256, L), vmem(2, 2, 16, L), vmem(19, 4, 2, 2 * L),
                vmem(2, FIELDS, 24, L), vmem(2, 18, 2, L), vmem(2, 18, 2, L),
                vmem(2, 18, 4, L), vmem(2, 18, 4, L), vmem(2, 20, L), vmem(2, 20, L),
                vmem(2, 80, L), vmem(19, 2, 24, L),
                dma(), dma(),
                dma(10), dma(10), dma(8), dma(8),
                dma(2), dma(2), dma(2), dma(2), dma(2), dma(2),
                dma(), dma(), dma(), dma(),
            ],
            compiler_params=pltpu.CompilerParams(
                collective_id=0, has_side_effects=True, vmem_limit_bytes=16 * 2**20
            ),
        )(density, populations)
        return pl.pallas_call(
            put,
            out_shape=shapes,
            in_specs=[any_spec, any_spec],
            out_specs=(any_spec, any_spec),
            scratch_shapes=[dma(), dma()],
            compiler_params=pltpu.CompilerParams(vmem_limit_bytes=8 * 2**20),
        )(density, populations)

    return jax.shard_map(
        local,
        mesh=mesh,
        in_specs=(P("gx", "gy", None), P(None, "gx", "gy", None)),
        out_specs=(P("gx", "gy", None), P(None, "gx", "gy", None)),
        check_vma=False,
    )
```

```python
import jax
import jax.numpy as jnp
from jax import lax
from jax.experimental import pallas as pl
from jax.experimental.pallas import tpu as pltpu
from jax.sharding import PartitionSpec as P

MESH = pl.DeviceIdType.MESH
EXACT = lax.Precision.HIGHEST
F32 = jnp.float32

TIME_STEP = 0.0008
FORCE_UNIT = 0.005
SPEED_UNIT = 2000.0
RELAX_TIME = 0.8
QUENCH = -0.25

SPEEDS = [
    (0, 0, 0),
    (1, 0, 0), (-1, 0, 0), (0, 1, 0), (0, -1, 0), (0, 0, 1), (0, 0, -1),
    (1, 1, 0), (-1, -1, 0), (1, -1, 0), (-1, 1, 0),
    (1, 0, 1), (-1, 0, -1), (1, 0, -1), (-1, 0, 1),
    (0, 1, 1), (0, -1, -1), (0, 1, -1), (0, -1, 1),
]
WEIGHTS = [1.0 / 3.0] + [1.0 / 18.0] * 6 + [1.0 / 36.0] * 12

MASS = 19
FIELDS = 23
RISE_X = [q for q in range(19) if SPEEDS[q][0] == 1]
FALL_X = [q for q in range(19) if SPEEDS[q][0] == -1]
RISE_Z = [q for q in range(19) if SPEEDS[q][2] == 1]
FALL_Z = [q for q in range(19) if SPEEDS[q][2] == -1]
MOMENTS = [MASS, MASS + 1, MASS + 2, MASS + 3]
DIAGONALS = [(1, 1), (1, -1), (-1, 1), (-1, -1)]


def dot_t(a, b):
    return lax.dot_general(
        a, b, (((1,), (1,)), ((), ())), precision=EXACT, preferred_element_type=F32
    )


def t_dot(a, b):
    return lax.dot_general(
        a, b, (((0,), (0,)), ((), ())), precision=EXACT, preferred_element_type=F32
    )


def iota(shape, dim):
    return lax.broadcasted_iota(jnp.int32, shape, dim)


def kernel(
    nx, n, dens_hbm, pops_hbm, OD, OP,
    E, E1, L1, PT, FA, FB, SP, SF, RF, SM, RM, MQ, MX, PV, EP, XS, XR, ZS, ZR, DS, DR, FR, RS,
    dsem, psem, h1_s, h1_r, h2_s, h2_r, px_s, px_r, pz_s, pz_r, pd_s, pd_r,
    ms_s, ms_r, fs_s, fs_r,
):
    L = 4 * n
    gx = lax.axis_index("gx")
    gy = lax.axis_index("gy")

    def place(sx, sy):
        return {"gx": lax.rem(gx + sx + nx, nx), "gy": lax.rem(gy + sy + n, n)}

    barrier = pltpu.get_barrier_semaphore()
    for sx, sy in ((1, 0), (-1, 0)):
        pl.semaphore_signal(barrier, inc=1, device_id=place(sx, sy), device_id_type=MESH)

    @pl.loop(1, n)
    def _(k):
        pl.semaphore_signal(barrier, inc=1, device_id=place(0, k), device_id_type=MESH)

    dens_in = pltpu.make_async_copy(dens_hbm, E.at[pl.ds(5, 8), pl.ds(8, 16)], dsem)
    dens_in.start()
    pops_in = pltpu.make_async_copy(pops_hbm, PV, psem)
    pops_in.start()

    def remote(src, dst, send, recv, where):
        return pltpu.make_async_remote_copy(
            src_ref=src, dst_ref=dst, send_sem=send, recv_sem=recv, device_id=where,
            device_id_type=MESH,
        )

    lane = iota((1, L), 1)

    pops_in.wait()
    for h in range(2):
        for member in range(19):
            for x in range(4):
                EP[h, member, pl.ds(x * 4 + 5, 2), :] = PV[member, x, :, pl.ds(h * L, L)]
        total = jnp.zeros((24, L), F32)
        moment = [jnp.zeros((24, L), F32) for _ in range(3)]
        for member in range(19):
            value = EP[h, member]
            total = total + value
            for c in range(3):
                if SPEEDS[member][c] == 1:
                    moment[c] = moment[c] + value
                elif SPEEDS[member][c] == -1:
                    moment[c] = moment[c] - value
        EP[h, MASS] = total
        for c in range(3):
            EP[h, MASS + 1 + c] = moment[c]

    for way, (members, row) in enumerate(((RISE_X, 17), (FALL_X, 5))):
        for f, field in enumerate(members + MOMENTS):
            for h in range(2):
                XS[way, f * 2 + h] = EP[h, field, pl.ds(row, 2), :]
    for way, (members, zi) in enumerate(((RISE_Z, 2), (FALL_Z, 1))):
        for f, field in enumerate(members + MOMENTS):
            for h in range(2):
                ZS[way, f * 2 + h] = EP[h, field, pl.ds(4 + zi, 4, stride=4), :]
    spread = [
        jnp.where((iota((n, L), 1) + h * L) // 8 == iota((n, L), 0), 1.0, 0.0).astype(F32)
        for h in range(2)
    ]
    for zl in range(2):
        result = None
        for h in range(2):
            for c in range(4):
                MX[zl, h, pl.ds(c * 4, 4), :] = EP[h, MASS + c, pl.ds(5 + zl, 4, stride=4), :]
            values = MX[zl, h]
            tiles = jnp.concatenate(
                [jnp.where(lax.rem(lane, 8) == y, values, 0.0) for y in range(8)], axis=0
            )
            part = dot_t(spread[h], tiles)
            result = part if result is None else result + part
        SM[pl.ds(zl, n, stride=8), :] = result

    dens_in.wait()
    pl.semaphore_wait(barrier, n + 1)

    def boxes(buf, items, first, send, recv):
        copies = []
        for i, (where, x0, x1, xs, y0, y1, ys) in enumerate(items):
            copies.append(remote(
                buf.at[pl.ds(x0, xs), pl.ds(y0, ys)], buf.at[pl.ds(x1, xs), pl.ds(y1, ys)],
                send.at[first + i], recv.at[first + i], place(*where),
            ))
        for copy in copies:
            copy.start()
        return copies

    def others():
        return [lax.rem(gy + (k * (n // 2 + 1)) % n, n) for k in range(1, n)]

    def to_all(src, dst, rows, send, recv):
        for to in others():
            remote(
                src.at[pl.ds(pl.multiple_of(to * 8, 8), rows)],
                dst.at[pl.ds(pl.multiple_of(gy * 8, 8), rows)],
                send, recv, {"gx": gx, "gy": to},
            ).start()
        for slot in range(rows):
            dst[pl.ds(gy * 8 + slot, 1), :] = src[pl.ds(gy * 8 + slot, 1), :]

    def wait_all(buf, rows, sem):
        whole = buf.at[pl.ds(0, (n - 1) * rows)]
        pltpu.make_async_copy(whole, whole, sem).wait()

    near = boxes(
        E, [((1, 0), 10, 2, 3, 8, 8, 16), ((-1, 0), 5, 13, 3, 8, 8, 16)], 0, h1_s, h1_r
    )
    rows = boxes(
        E, [((0, 1), 5, 5, 8, 21, 5, 3), ((0, -1), 5, 5, 8, 8, 24, 3)], 2, h1_s, h1_r
    )
    far = boxes(
        E, [((1, 0), 8, 0, 2, 8, 8, 16), ((-1, 0), 8, 16, 2, 8, 8, 16)], 4, h1_s, h1_r
    )
    to_all(SM, RM, 2, ms_s, ms_r)
    face_z = [
        remote(ZS.at[0], ZR.at[0], pz_s.at[0], pz_r.at[0], place(0, 1)),
        remote(ZS.at[1], ZR.at[1], pz_s.at[1], pz_r.at[1], place(0, -1)),
    ]
    face_x = [
        remote(XS.at[0], XR.at[0], px_s.at[0], px_r.at[0], place(1, 0)),
        remote(XS.at[1], XR.at[1], px_s.at[1], px_r.at[1], place(-1, 0)),
    ]
    for copy in face_z + face_x:
        copy.start()

    for copy in rows:
        copy.wait_recv()
    corners = boxes(
        E,
        [
            (where, x0, x1, 4, y0, y0, 3)
            for where, x0, x1 in (((1, 0), 9, 1), ((-1, 0), 5, 13)) for y0 in (5, 24)
        ],
        6, h1_s, h1_r,
    )
    for way in range(2):
        face_z[way].wait_recv()
    for way, (sx, x) in enumerate(((1, 3), (-1, 0))):
        for side, members in enumerate((RISE_Z, FALL_Z)):
            member = SPEEDS.index((sx, 0, 1 - 2 * side))
            for f, item in enumerate([members.index(member), 5, 6, 7, 8]):
                for h in range(2):
                    DS[way, pl.ds((side * 5 + f) * 2 + h, 1), :] = ZR[
                        side, item * 2 + h, pl.ds(x, 1), :
                    ]
    edges = [
        remote(DS.at[0], DR.at[0], pd_s.at[0], pd_r.at[0], place(1, 0)),
        remote(DS.at[1], DR.at[1], pd_s.at[1], pd_r.at[1], place(-1, 0)),
    ]
    for copy in edges:
        copy.start()
    for way, (members, zi) in enumerate(((RISE_Z, 0), (FALL_Z, 3))):
        for f, field in enumerate(members + MOMENTS):
            for h in range(2):
                EP[h, field, pl.ds(4 + zi, 4, stride=4), :] = ZR[way, f * 2 + h]

    def turn(value, by):
        return pltpu.roll(value, by % L, 1)

    def lap(ref, i, r0, rows):
        c = ref[i, pl.ds(r0, rows), :]
        return c, (
            -6.0 * c + ref[i - 1, pl.ds(r0, rows), :] + ref[i + 1, pl.ds(r0, rows), :]
            + ref[i, pl.ds(r0 - 1, rows), :] + ref[i, pl.ds(r0 + 1, rows), :]
            + turn(c, 1) + turn(c, -1)
        )

    def potential(src, outer, inner, r0, rows):
        for i in outer:
            L1[i, pl.ds(0, rows), :] = lap(src, i + 1, r0, rows)[1]
        for j in inner:
            c, second = lap(L1, j + 1, 1, rows)
            rho = src[j + 2, pl.ds(r0 + 1, rows), :]
            PT[j, pl.ds(0, rows), :] = (
                (QUENCH + 1.0) * rho + 2.0 * c + second + rho * rho * rho
            )

    wait_all(RM, 2, ms_r)
    shape = (2 * n, L)
    row = iota(shape, 0)
    pick = iota(shape, 1) // 2 == 2 * lax.rem(row, n) + row // n
    both = jnp.concatenate([RM[pl.ds(zl, n, stride=8), :] for zl in range(2)], axis=0)
    wide = t_dot(both, jnp.where(pick, 1.0, 0.0).astype(F32))
    for y in range(16):
        MQ[pl.ds(y * 16, 16), :] = wide[(y // 2) * 16:(y // 2 + 1) * 16]

    potential(E, range(5, 11), range(5, 9), 6, 24)
    for copy in near + corners:
        copy.wait_recv()
    potential(E, (2, 3, 4, 11, 12, 13), (2, 3, 4, 9, 10, 11), 6, 24)

    scale = -0.5 * FORCE_UNIT * 0.125
    zeros = jnp.zeros((16, L), F32)
    for extra in range(8, 16):
        FB[pl.ds(extra, 16, stride=16), :] = zeros

    def force_pair(src, e0, p0, r0, rows):
        sums = [None, None, None]
        for k in range(2):
            rho = src[e0 + k, pl.ds(r0, rows), :] * scale
            mid = PT[p0 + k, pl.ds(1, rows), :]
            parts = (
                PT[p0 + k + 1, pl.ds(1, rows), :] - PT[p0 + k - 1, pl.ds(1, rows), :],
                PT[p0 + k, pl.ds(2, rows), :] - PT[p0 + k, pl.ds(0, rows), :],
                turn(mid, -1) - turn(mid, 1),
            )
            for c in range(3):
                value = rho * parts[c]
                sums[c] = value if sums[c] is None else sums[c] + value
        return sums

    def outgoing(xi):
        sums = force_pair(E, 2 * xi + 3, 2 * xi + 1, 8, 16)
        for c in range(3):
            cx = c * 6 + xi
            if 1 <= xi <= 4:
                SP[c * 4 + xi - 1] = sums[c]
            if cx < 16:
                FA[pl.ds(cx, 16, stride=16), :] = sums[c]
            else:
                for zl in range(4):
                    FB[pl.ds((cx - 16) * 4 + zl, 16, stride=16), :] = turn(
                        sums[c], -2 * (zl - 1)
                    )

    for xi in range(1, 5):
        outgoing(xi)

    even_y = lax.rem(iota((16, L), 0), 2) == 0
    even_z = lax.rem(iota((16, L), 1), 2) == 0

    def fine_speed(x):
        mass = MQ[pl.ds(x, 16, stride=16), :]
        inverse = SPEED_UNIT * 0.5 / mass
        out = []
        for c in range(3):
            s = SP[c * 4 + x]
            s = s + jnp.where(even_y, pltpu.roll(s, 15, 0), pltpu.roll(s, 1, 0))
            s = s + jnp.where(even_z, turn(s, -1), turn(s, 1))
            m = MQ[pl.ds((c + 1) * 4 + x, 16, stride=16), :]
            out.append((m + 0.5 * s) * inverse)
        return out

    def advance(src, e, p, speed):
        mid = src[e, pl.ds(8, 16), :]
        advect = (
            speed[0] * (src[e + 1, pl.ds(8, 16), :] - src[e - 1, pl.ds(8, 16), :])
            + speed[1] * (src[e, pl.ds(9, 16), :] - src[e, pl.ds(7, 16), :])
            + speed[2] * (turn(mid, -1) - turn(mid, 1))
        )
        return mid + TIME_STEP * (lap(PT, p, 1, 16)[1] - advect)

    for x in range(4):
        speed = fine_speed(x)
        for c in range(3):
            SP[c * 4 + x] = speed[c]
        for k in (2 * x, 2 * x + 1):
            E1[k + 3, pl.ds(8, 16), :] = advance(E, k + 5, k + 3, speed)
    again = boxes(
        E1,
        [
            ((sx, sy), *((9, 1, 2) if sx == 1 else (3, 11, 2)),
             *((22, 6, 2) if sy == 1 else (8, 24, 2)))
            for sx, sy in DIAGONALS
        ] + [
            ((1, 0), 8, 0, 3, 8, 8, 16),
            ((-1, 0), 3, 11, 3, 8, 8, 16),
            ((0, 1), 3, 3, 8, 21, 5, 3),
            ((0, -1), 3, 3, 8, 8, 24, 3),
        ],
        0, h2_s, h2_r,
    )

    for copy in far:
        copy.wait_recv()
    potential(E, (0, 1, 14, 15), (0, 1, 12, 13), 6, 24)
    for xi in (0, 5):
        outgoing(xi)

    shape = (4 * n, L)
    row = iota(shape, 0)
    window = lax.rem(2 * lax.rem(row, n) - 1 + row // n + 2 * n, 2 * n)
    choose = jnp.where(iota(shape, 1) // 2 == window, 1.0, 0.0).astype(F32)
    ga = jnp.concatenate(
        [FA[pl.ds(32 * y, 16), :] + FA[pl.ds(32 * y + 16, 16), :] for y in range(8)], axis=0
    )
    gb = jnp.concatenate(
        [FB[pl.ds(32 * y, 16), :] + FB[pl.ds(32 * y + 16, 16), :] for y in range(8)], axis=0
    )
    ta = dot_t(choose, ga)
    tb = dot_t(choose[n:2 * n], gb)
    for zl in range(4):
        SF[pl.ds(zl, n, stride=8), :] = ta[zl * n:(zl + 1) * n]
    SF[pl.ds(4, n, stride=8), :] = tb

    to_all(SF, RF, 5, fs_s, fs_r)

    for way in range(2):
        face_x[way].wait_recv()
    for way, (members, row) in enumerate(((RISE_X, 1), (FALL_X, 21))):
        for f, field in enumerate(members + MOMENTS):
            for h in range(2):
                EP[h, field, pl.ds(row, 2), :] = XR[way, f * 2 + h]
    for way in range(2):
        edges[way].wait_recv()
        for side, members in enumerate((RISE_Z, FALL_Z)):
            member = SPEEDS.index((1 - 2 * way, 0, 1 - 2 * side))
            row = way * 20 + side * 3
            for f, field in enumerate([member] + MOMENTS):
                for h in range(2):
                    EP[h, field, pl.ds(row, 1), :] = DR[way, pl.ds((side * 5 + f) * 2 + h, 1), :]

    for copy in again:
        copy.wait_recv()
    potential(E1, range(12), range(10), 6, 24)
    for x in range(4):
        speed = [SP[c * 4 + x] for c in range(3)]
        for k in (2 * x, 2 * x + 1):
            OD[k] = advance(E1, k + 3, k + 1, speed)

    wait_all(RF, 5, fs_r)
    half = n // 2
    expand = jnp.where(iota((half, L), 1) // 8 == iota((half, L), 0), 1.0, 0.0).astype(F32)
    for slot in range(5):
        whole = RF[pl.ds(slot, n, stride=8), :]
        for h in range(2):
            q = t_dot(whole[h * half:(h + 1) * half], expand)
            value = q[0:16]
            for y in range(1, 8):
                value = jnp.where(lax.rem(lane, 8) == y, q[y * 16:(y + 1) * 16], value)
            if slot < 4:
                FR[h, pl.ds(slot, 16, stride=4), :] = value
            else:
                FR[h, pl.ds(64, 16), :] = value

    rate = 1.0 / RELAX_TIME
    gain = 1.0 - 0.5 / RELAX_TIME
    state = []
    for h in range(2):
        mass = EP[h, MASS]
        inverse = 1.0 / mass
        force = [FR[h, pl.ds(c * 24, 24), :] for c in range(3)]
        flow = [(EP[h, MASS + 1 + c] + 0.5 * force[c]) * inverse for c in range(3)]
        square = flow[0] * flow[0] + flow[1] * flow[1] + flow[2] * flow[2]
        work = flow[0] * force[0] + flow[1] * force[1] + flow[2] * force[2]
        common = rate * mass * (1.0 - 1.5 * square) - (3.0 * gain) * work
        state.append((3.0 * rate * mass, force, flow, common))

    def along(speed, vector):
        out = None
        for c in range(3):
            if speed[c] == 1:
                out = vector[c] if out is None else out + vector[c]
            elif speed[c] == -1:
                out = -vector[c] if out is None else out - vector[c]
        return out

    def passed(member, parts):
        cx, cy, cz = SPEEDS[member]
        parts = [EP[h, member] * (1.0 - rate) + parts[h] for h in range(2)]
        if cy:
            turned = [pltpu.roll(v, cy % L, 1) for v in parts]
            edge = lane == (0 if cy == 1 else L - 1)
            parts = [jnp.where(edge, turned[1 - h], turned[h]) for h in range(2)]
        for h in range(2):
            RS[member, h] = parts[h]
            for x in range(4):
                OP[member, x, :, pl.ds(h * L, L)] = RS[
                    member, h, pl.ds((x + 1 - cx) * 4 + 1 - cz, 2), :
                ]

    passed(0, [WEIGHTS[0] * state[h][3] for h in range(2)])
    scaled = {}
    for w in (WEIGHTS[1], WEIGHTS[7]):
        scaled[w] = [(w * state[h][0], w * state[h][3]) for h in range(2)]
    for member in range(1, 19, 2):
        w = WEIGHTS[member]
        plus, minus = [], []
        for h in range(2):
            mass, common = scaled[w][h]
            cu, cf = along(SPEEDS[member], state[h][2]), along(SPEEDS[member], state[h][1])
            first, second = mass * cu, (3.0 * gain * w) * cf
            odd = first + second
            even = common + cu * (1.5 * first + 3.0 * second)
            plus.append(even + odd)
            minus.append(even - odd)
        passed(member, plus)
        passed(member + 1, minus)

    for copy in near + rows + far + corners + again + face_x + face_z + edges:
        copy.wait_send()
    wait_all(SM, 2, ms_s)
    wait_all(SF, 5, fs_s)


def put(dens, pops, dens_out, pops_out, dsem, psem):
    first = pltpu.make_async_copy(dens, dens_out, dsem)
    second = pltpu.make_async_copy(pops, pops_out, psem)
    second.start()
    first.start()
    first.wait()
    second.wait()


def solution(mesh):
    nx, n = mesh.shape["gx"], mesh.shape["gy"]
    L = 4 * n

    def local(density, populations):
        vmem = lambda *shape: pltpu.VMEM(shape, F32)
        dma = lambda *shape: pltpu.SemaphoreType.DMA(shape)
        any_spec = pl.BlockSpec(memory_space=pl.ANY)
        vmem_spec = pl.BlockSpec(memory_space=pltpu.VMEM)
        shapes = (
            jax.ShapeDtypeStruct((8, 16, L), F32),
            jax.ShapeDtypeStruct((19, 4, 2, 2 * L), F32),
        )
        density = pltpu.with_memory_space_constraint(density, pltpu.HBM)
        populations = pltpu.with_memory_space_constraint(populations, pltpu.HBM)
        density, populations = pl.pallas_call(
            lambda *refs: kernel(nx, n, *refs),
            out_shape=shapes,
            in_specs=[any_spec, any_spec],
            out_specs=(vmem_spec, vmem_spec),
            scratch_shapes=[
                vmem(18, 32, L), vmem(14, 32, L), vmem(16, 32, L), vmem(14, 32, L),
                vmem(256, L), vmem(256, L), vmem(12, 16, L),
                vmem(n * 8, 128), vmem(n * 8, 128), vmem(n * 8, 128), vmem(n * 8, 128),
                vmem(256, L), vmem(2, 2, 16, L), vmem(19, 4, 2, 2 * L),
                vmem(2, FIELDS, 24, L), vmem(2, 18, 2, L), vmem(2, 18, 2, L),
                vmem(2, 18, 4, L), vmem(2, 18, 4, L), vmem(2, 20, L), vmem(2, 20, L),
                vmem(2, 80, L), vmem(19, 2, 24, L),
                dma(), dma(),
                dma(10), dma(10), dma(8), dma(8),
                dma(2), dma(2), dma(2), dma(2), dma(2), dma(2),
                dma(), dma(), dma(), dma(),
            ],
            compiler_params=pltpu.CompilerParams(
                collective_id=0, has_side_effects=True, vmem_limit_bytes=16 * 2**20
            ),
        )(density, populations)
        return pl.pallas_call(
            put,
            out_shape=shapes,
            in_specs=[any_spec, any_spec],
            out_specs=(any_spec, any_spec),
            scratch_shapes=[dma(), dma()],
            compiler_params=pltpu.CompilerParams(vmem_limit_bytes=8 * 2**20),
        )(density, populations)

    return jax.shard_map(
        local,
        mesh=mesh,
        in_specs=(P("gx", "gy", None), P(None, "gx", "gy", None)),
        out_specs=(P("gx", "gy", None), P(None, "gx", "gy", None)),
        check_vma=False,
    )
```

```python
import jax
import jax.numpy as jnp
from jax import lax
from jax.experimental import pallas as pl
from jax.experimental.pallas import tpu as pltpu
from jax.sharding import PartitionSpec as P

MESH = pl.DeviceIdType.MESH
EXACT = lax.Precision.HIGHEST
F32 = jnp.float32

TIME_STEP = 0.0008
FORCE_UNIT = 0.005
SPEED_UNIT = 2000.0
RELAX_TIME = 0.8
QUENCH = -0.25

SPEEDS = [
    (0, 0, 0),
    (1, 0, 0), (-1, 0, 0), (0, 1, 0), (0, -1, 0), (0, 0, 1), (0, 0, -1),
    (1, 1, 0), (-1, -1, 0), (1, -1, 0), (-1, 1, 0),
    (1, 0, 1), (-1, 0, -1), (1, 0, -1), (-1, 0, 1),
    (0, 1, 1), (0, -1, -1), (0, 1, -1), (0, -1, 1),
]
WEIGHTS = [1.0 / 3.0] + [1.0 / 18.0] * 6 + [1.0 / 36.0] * 12

MASS = 19
FIELDS = 24
RISE_X = [q for q in range(19) if SPEEDS[q][0] == 1]
FALL_X = [q for q in range(19) if SPEEDS[q][0] == -1]
RISE_Z = [q for q in range(19) if SPEEDS[q][2] == 1]
FALL_Z = [q for q in range(19) if SPEEDS[q][2] == -1]
MOMENTS = [MASS, MASS + 1, MASS + 2, MASS + 3]
DIAGONALS = [(1, 1), (1, -1), (-1, 1), (-1, -1)]


def dot_t(a, b):
    return lax.dot_general(
        a, b, (((1,), (1,)), ((), ())), precision=EXACT, preferred_element_type=F32
    )


def t_dot(a, b):
    return lax.dot_general(
        a, b, (((0,), (0,)), ((), ())), precision=EXACT, preferred_element_type=F32
    )


def iota(shape, dim):
    return lax.broadcasted_iota(jnp.int32, shape, dim)


def kernel(
    nx, n, dens_hbm, pops_hbm, OD, OP,
    E, E1, L1, PT, FA, FB, SP, SF, RF, SM, RM, MQ, MX, PV, EP, XS, XR, ZS, ZR, DS, DR, FR, RS,
    dsem, psem, h1_s, h1_r, h2_s, h2_r, px_s, px_r, pz_s, pz_r, pd_s, pd_r,
    ms_s, ms_r, fs_s, fs_r,
):
    L = 4 * n
    gx = lax.axis_index("gx")
    gy = lax.axis_index("gy")

    def place(sx, sy):
        return {"gx": lax.rem(gx + sx + nx, nx), "gy": lax.rem(gy + sy + n, n)}

    barrier = pltpu.get_barrier_semaphore()
    for sx, sy in ((1, 0), (-1, 0)):
        pl.semaphore_signal(barrier, inc=1, device_id=place(sx, sy), device_id_type=MESH)

    @pl.loop(1, n)
    def _(k):
        pl.semaphore_signal(barrier, inc=1, device_id=place(0, k), device_id_type=MESH)

    dens_in = pltpu.make_async_copy(dens_hbm, E.at[pl.ds(5, 8), pl.ds(8, 16)], dsem)
    dens_in.start()
    pops_in = pltpu.make_async_copy(pops_hbm, PV.at[pl.ds(0, 19)], psem)
    pops_in.start()

    def remote(src, dst, send, recv, where):
        return pltpu.make_async_remote_copy(
            src_ref=src, dst_ref=dst, send_sem=send, recv_sem=recv, device_id=where,
            device_id_type=MESH,
        )

    lane = iota((1, L), 1)

    pops_in.wait()
    for h in range(2):
        for member in range(19):
            for x in range(4):
                EP[h, member, pl.ds(x * 4 + 5, 2), :] = PV[member, x, :, pl.ds(h * L, L)]
        total = jnp.zeros((24, L), F32)
        moment = [jnp.zeros((24, L), F32) for _ in range(3)]
        for member in range(19):
            value = EP[h, member]
            total = total + value
            for c in range(3):
                if SPEEDS[member][c] == 1:
                    moment[c] = moment[c] + value
                elif SPEEDS[member][c] == -1:
                    moment[c] = moment[c] - value
        EP[h, MASS] = total
        for c in range(3):
            EP[h, MASS + 1 + c] = moment[c]

    for way, (members, row) in enumerate(((RISE_X, 17), (FALL_X, 5))):
        for f, field in enumerate(members + MOMENTS):
            for h in range(2):
                XS[way, f * 2 + h] = EP[h, field, pl.ds(row, 2), :]
    for way, (members, zi) in enumerate(((RISE_Z, 2), (FALL_Z, 1))):
        for f, field in enumerate(members + MOMENTS):
            for h in range(2):
                ZS[way, f * 2 + h] = EP[h, field, pl.ds(4 + zi, 4, stride=4), :]
    spread = [
        jnp.where((iota((n, L), 1) + h * L) // 8 == iota((n, L), 0), 1.0, 0.0).astype(F32)
        for h in range(2)
    ]
    for zl in range(2):
        result = None
        for h in range(2):
            for c in range(4):
                MX[zl, h, pl.ds(c * 4, 4), :] = EP[h, MASS + c, pl.ds(5 + zl, 4, stride=4), :]
            values = MX[zl, h]
            tiles = jnp.concatenate(
                [jnp.where(lax.rem(lane, 8) == y, values, 0.0) for y in range(8)], axis=0
            )
            part = dot_t(spread[h], tiles)
            result = part if result is None else result + part
        SM[pl.ds(zl, n, stride=8), :] = result

    dens_in.wait()
    pl.semaphore_wait(barrier, n + 1)

    def boxes(buf, items, first, send, recv):
        copies = []
        for i, (where, x0, x1, xs, y0, y1, ys) in enumerate(items):
            copies.append(remote(
                buf.at[pl.ds(x0, xs), pl.ds(y0, ys)], buf.at[pl.ds(x1, xs), pl.ds(y1, ys)],
                send.at[first + i], recv.at[first + i], place(*where),
            ))
        for copy in copies:
            copy.start()
        return copies

    def others():
        return [lax.rem(gy + (k * (n // 2 + 1)) % n, n) for k in range(1, n)]

    def to_all(src, dst, rows, send, recv):
        for to in others():
            remote(
                src.at[pl.ds(pl.multiple_of(to * 8, 8), rows)],
                dst.at[pl.ds(pl.multiple_of(gy * 8, 8), rows)],
                send, recv, {"gx": gx, "gy": to},
            ).start()
        for slot in range(rows):
            dst[pl.ds(gy * 8 + slot, 1), :] = src[pl.ds(gy * 8 + slot, 1), :]

    def wait_all(buf, rows, sem):
        whole = buf.at[pl.ds(0, (n - 1) * rows)]
        pltpu.make_async_copy(whole, whole, sem).wait()

    near = boxes(
        E, [((1, 0), 10, 2, 3, 8, 8, 16), ((-1, 0), 5, 13, 3, 8, 8, 16)], 0, h1_s, h1_r
    )
    rows = boxes(
        E, [((0, 1), 5, 5, 8, 21, 5, 3), ((0, -1), 5, 5, 8, 8, 24, 3)], 2, h1_s, h1_r
    )
    far = boxes(
        E, [((1, 0), 8, 0, 2, 8, 8, 16), ((-1, 0), 8, 16, 2, 8, 8, 16)], 4, h1_s, h1_r
    )
    to_all(SM, RM, 2, ms_s, ms_r)
    face_z = [
        remote(ZS.at[0], ZR.at[0], pz_s.at[0], pz_r.at[0], place(0, 1)),
        remote(ZS.at[1], ZR.at[1], pz_s.at[1], pz_r.at[1], place(0, -1)),
    ]
    face_x = [
        remote(XS.at[0], XR.at[0], px_s.at[0], px_r.at[0], place(1, 0)),
        remote(XS.at[1], XR.at[1], px_s.at[1], px_r.at[1], place(-1, 0)),
    ]
    for copy in face_z + face_x:
        copy.start()

    for copy in rows:
        copy.wait_recv()
    corners = boxes(
        E,
        [
            (where, x0, x1, 4, y0, y0, 3)
            for where, x0, x1 in (((1, 0), 9, 1), ((-1, 0), 5, 13)) for y0 in (5, 24)
        ],
        6, h1_s, h1_r,
    )
    for way in range(2):
        face_z[way].wait_recv()
    for way, (sx, x) in enumerate(((1, 3), (-1, 0))):
        for side, members in enumerate((RISE_Z, FALL_Z)):
            member = SPEEDS.index((sx, 0, 1 - 2 * side))
            for f, item in enumerate([members.index(member), 5, 6, 7, 8]):
                for h in range(2):
                    DS[way, pl.ds((side * 5 + f) * 2 + h, 1), :] = ZR[
                        side, item * 2 + h, pl.ds(x, 1), :
                    ]
    edges = [
        remote(DS.at[0], DR.at[0], pd_s.at[0], pd_r.at[0], place(1, 0)),
        remote(DS.at[1], DR.at[1], pd_s.at[1], pd_r.at[1], place(-1, 0)),
    ]
    for copy in edges:
        copy.start()
    for way, (members, zi) in enumerate(((RISE_Z, 0), (FALL_Z, 3))):
        for f, field in enumerate(members + MOMENTS):
            for h in range(2):
                EP[h, field, pl.ds(4 + zi, 4, stride=4), :] = ZR[way, f * 2 + h]

    def turn(value, by):
        return pltpu.roll(value, by % L, 1)

    def lap(ref, i, r0, rows):
        c = ref[i, pl.ds(r0, rows), :]
        return c, (
            -6.0 * c + ref[i - 1, pl.ds(r0, rows), :] + ref[i + 1, pl.ds(r0, rows), :]
            + ref[i, pl.ds(r0 - 1, rows), :] + ref[i, pl.ds(r0 + 1, rows), :]
            + turn(c, 1) + turn(c, -1)
        )

    def potential(src, outer, inner, r0, rows):
        for i in outer:
            L1[i, pl.ds(0, rows), :] = lap(src, i + 1, r0, rows)[1]
        for j in inner:
            c, second = lap(L1, j + 1, 1, rows)
            rho = src[j + 2, pl.ds(r0 + 1, rows), :]
            PT[j, pl.ds(0, rows), :] = (
                (QUENCH + 1.0) * rho + 2.0 * c + second + rho * rho * rho
            )

    wait_all(RM, 2, ms_r)
    shape = (2 * n, L)
    row = iota(shape, 0)
    pick = iota(shape, 1) // 2 == 2 * lax.rem(row, n) + row // n
    both = jnp.concatenate([RM[pl.ds(zl, n, stride=8), :] for zl in range(2)], axis=0)
    wide = t_dot(both, jnp.where(pick, 1.0, 0.0).astype(F32))
    for y in range(16):
        MQ[pl.ds(y * 16, 16), :] = wide[(y // 2) * 16:(y // 2 + 1) * 16]

    potential(E, range(5, 11), range(5, 9), 6, 24)
    for copy in near + corners:
        copy.wait_recv()
    potential(E, (2, 3, 4, 11, 12, 13), (2, 3, 4, 9, 10, 11), 6, 24)

    scale = -0.5 * FORCE_UNIT * 0.125
    zeros = jnp.zeros((16, L), F32)
    for extra in range(8, 16):
        FB[pl.ds(extra, 16, stride=16), :] = zeros

    def force_pair(src, e0, p0, r0, rows):
        sums = [None, None, None]
        for k in range(2):
            rho = src[e0 + k, pl.ds(r0, rows), :] * scale
            mid = PT[p0 + k, pl.ds(1, rows), :]
            parts = (
                PT[p0 + k + 1, pl.ds(1, rows), :] - PT[p0 + k - 1, pl.ds(1, rows), :],
                PT[p0 + k, pl.ds(2, rows), :] - PT[p0 + k, pl.ds(0, rows), :],
                turn(mid, -1) - turn(mid, 1),
            )
            for c in range(3):
                value = rho * parts[c]
                sums[c] = value if sums[c] is None else sums[c] + value
        return sums

    def outgoing(xi):
        sums = force_pair(E, 2 * xi + 3, 2 * xi + 1, 8, 16)
        for c in range(3):
            cx = c * 6 + xi
            if 1 <= xi <= 4:
                SP[c * 4 + xi - 1] = sums[c]
            if cx < 16:
                FA[pl.ds(cx, 16, stride=16), :] = sums[c]
            else:
                for zl in range(4):
                    FB[pl.ds((cx - 16) * 4 + zl, 16, stride=16), :] = turn(
                        sums[c], -2 * (zl - 1)
                    )

    for xi in range(1, 5):
        outgoing(xi)

    even_y = lax.rem(iota((16, L), 0), 2) == 0
    even_z = lax.rem(iota((16, L), 1), 2) == 0

    def fine_speed(x):
        mass = MQ[pl.ds(x, 16, stride=16), :]
        inverse = SPEED_UNIT * 0.5 / mass
        out = []
        for c in range(3):
            s = SP[c * 4 + x]
            s = s + jnp.where(even_y, pltpu.roll(s, 15, 0), pltpu.roll(s, 1, 0))
            s = s + jnp.where(even_z, turn(s, -1), turn(s, 1))
            m = MQ[pl.ds((c + 1) * 4 + x, 16, stride=16), :]
            out.append((m + 0.5 * s) * inverse)
        return out

    def advance(src, e, p, speed):
        mid = src[e, pl.ds(8, 16), :]
        advect = (
            speed[0] * (src[e + 1, pl.ds(8, 16), :] - src[e - 1, pl.ds(8, 16), :])
            + speed[1] * (src[e, pl.ds(9, 16), :] - src[e, pl.ds(7, 16), :])
            + speed[2] * (turn(mid, -1) - turn(mid, 1))
        )
        return mid + TIME_STEP * (lap(PT, p, 1, 16)[1] - advect)

    for x in range(4):
        speed = fine_speed(x)
        for c in range(3):
            SP[c * 4 + x] = speed[c]
        for k in (2 * x, 2 * x + 1):
            E1[k + 3, pl.ds(8, 16), :] = advance(E, k + 5, k + 3, speed)
    again = boxes(
        E1,
        [
            ((sx, sy), *((9, 1, 2) if sx == 1 else (3, 11, 2)),
             *((22, 6, 2) if sy == 1 else (8, 24, 2)))
            for sx, sy in DIAGONALS
        ] + [
            ((1, 0), 8, 0, 3, 8, 8, 16),
            ((-1, 0), 3, 11, 3, 8, 8, 16),
            ((0, 1), 3, 3, 8, 21, 5, 3),
            ((0, -1), 3, 3, 8, 8, 24, 3),
        ],
        0, h2_s, h2_r,
    )

    for copy in far:
        copy.wait_recv()
    potential(E, (0, 1, 14, 15), (0, 1, 12, 13), 6, 24)
    for xi in (0, 5):
        outgoing(xi)

    shape = (4 * n, L)
    row = iota(shape, 0)
    window = lax.rem(2 * lax.rem(row, n) - 1 + row // n + 2 * n, 2 * n)
    choose = jnp.where(iota(shape, 1) // 2 == window, 1.0, 0.0).astype(F32)
    ga = jnp.concatenate(
        [FA[pl.ds(32 * y, 16), :] + FA[pl.ds(32 * y + 16, 16), :] for y in range(8)], axis=0
    )
    gb = jnp.concatenate(
        [FB[pl.ds(32 * y, 16), :] + FB[pl.ds(32 * y + 16, 16), :] for y in range(8)], axis=0
    )
    ta = dot_t(choose, ga)
    tb = dot_t(choose[n:2 * n], gb)
    for zl in range(4):
        SF[pl.ds(zl, n, stride=8), :] = ta[zl * n:(zl + 1) * n]
    SF[pl.ds(4, n, stride=8), :] = tb

    to_all(SF, RF, 5, fs_s, fs_r)

    for way in range(2):
        face_x[way].wait_recv()
    for way, (members, row) in enumerate(((RISE_X, 1), (FALL_X, 21))):
        for f, field in enumerate(members + MOMENTS):
            for h in range(2):
                EP[h, field, pl.ds(row, 2), :] = XR[way, f * 2 + h]
    for way in range(2):
        edges[way].wait_recv()
        for side, members in enumerate((RISE_Z, FALL_Z)):
            member = SPEEDS.index((1 - 2 * way, 0, 1 - 2 * side))
            row = way * 20 + side * 3
            for f, field in enumerate([member] + MOMENTS):
                for h in range(2):
                    EP[h, field, pl.ds(row, 1), :] = DR[way, pl.ds((side * 5 + f) * 2 + h, 1), :]

    for copy in again:
        copy.wait_recv()
    potential(E1, range(12), range(10), 6, 24)
    for x in range(4):
        speed = [SP[c * 4 + x] for c in range(3)]
        for k in (2 * x, 2 * x + 1):
            OD[k] = advance(E1, k + 3, k + 1, speed)

    wait_all(RF, 5, fs_r)
    half = n // 2
    expand = jnp.where(iota((half, L), 1) // 8 == iota((half, L), 0), 1.0, 0.0).astype(F32)
    for slot in range(5):
        whole = RF[pl.ds(slot, n, stride=8), :]
        for h in range(2):
            q = t_dot(whole[h * half:(h + 1) * half], expand)
            value = q[0:16]
            for y in range(1, 8):
                value = jnp.where(lax.rem(lane, 8) == y, q[y * 16:(y + 1) * 16], value)
            if slot < 4:
                FR[h, pl.ds(slot, 16, stride=4), :] = value
            else:
                FR[h, pl.ds(64, 16), :] = value

    rate = 1.0 / RELAX_TIME
    gain = 1.0 - 0.5 / RELAX_TIME
    state = []
    for h in range(2):
        mass = EP[h, MASS]
        inverse = 1.0 / mass
        force = [FR[h, pl.ds(c * 24, 24), :] for c in range(3)]
        flow = [(EP[h, MASS + 1 + c] + 0.5 * force[c]) * inverse for c in range(3)]
        square = flow[0] * flow[0] + flow[1] * flow[1] + flow[2] * flow[2]
        work = flow[0] * force[0] + flow[1] * force[1] + flow[2] * force[2]
        common = rate * mass * (1.0 - 1.5 * square) - (3.0 * gain) * work
        state.append((3.0 * rate * mass, force, flow, common))

    def along(speed, vector):
        out = None
        for c in range(3):
            if speed[c] == 1:
                out = vector[c] if out is None else out + vector[c]
            elif speed[c] == -1:
                out = -vector[c] if out is None else out - vector[c]
        return out

    def passed(member, parts):
        cx, cy, cz = SPEEDS[member]
        parts = [EP[h, member] * (1.0 - rate) + parts[h] for h in range(2)]
        if cy:
            turned = [pltpu.roll(v, cy % L, 1) for v in parts]
            edge = lane == (0 if cy == 1 else L - 1)
            parts = [jnp.where(edge, turned[1 - h], turned[h]) for h in range(2)]
        for h in range(2):
            RS[member, h] = parts[h]
            for x in range(4):
                OP[member, x, :, pl.ds(h * L, L)] = RS[
                    member, h, pl.ds((x + 1 - cx) * 4 + 1 - cz, 2), :
                ]

    passed(0, [WEIGHTS[0] * state[h][3] for h in range(2)])
    scaled = {}
    for w in (WEIGHTS[1], WEIGHTS[7]):
        scaled[w] = [(w * state[h][0], w * state[h][3]) for h in range(2)]
    for member in range(1, 19, 2):
        w = WEIGHTS[member]
        plus, minus = [], []
        for h in range(2):
            mass, common = scaled[w][h]
            cu, cf = along(SPEEDS[member], state[h][2]), along(SPEEDS[member], state[h][1])
            first, second = mass * cu, (3.0 * gain * w) * cf
            odd = first + second
            even = common + cu * (1.5 * first + 3.0 * second)
            plus.append(even + odd)
            minus.append(even - odd)
        passed(member, plus)
        passed(member + 1, minus)

    for copy in near + rows + far + corners + again + face_x + face_z + edges:
        copy.wait_send()
    wait_all(SM, 2, ms_s)
    wait_all(SF, 5, fs_s)


def put(dens, pops, dens_out, pops_out, dsem, psem):
    first = pltpu.make_async_copy(dens, dens_out, dsem)
    second = pltpu.make_async_copy(pops, pops_out, psem)
    second.start()
    first.start()
    first.wait()
    second.wait()


def solution(mesh):
    nx, n = mesh.shape["gx"], mesh.shape["gy"]
    L = 4 * n

    def local(density, populations):
        vmem = lambda *shape: pltpu.VMEM(shape, F32)
        dma = lambda *shape: pltpu.SemaphoreType.DMA(shape)
        any_spec = pl.BlockSpec(memory_space=pl.ANY)
        vmem_spec = pl.BlockSpec(memory_space=pltpu.VMEM)
        shapes = (
            jax.ShapeDtypeStruct((8, 16, L), F32),
            jax.ShapeDtypeStruct((19, 4, 2, 2 * L), F32),
        )
        density = pltpu.with_memory_space_constraint(density, pltpu.HBM)
        populations = pltpu.with_memory_space_constraint(populations, pltpu.HBM)
        density, populations = pl.pallas_call(
            lambda *refs: kernel(nx, n, *refs),
            out_shape=shapes,
            in_specs=[any_spec, any_spec],
            out_specs=(vmem_spec, vmem_spec),
            scratch_shapes=[
                vmem(18, 32, L), vmem(14, 32, L), vmem(16, 32, L), vmem(14, 32, L),
                vmem(256, L), vmem(256, L), vmem(12, 16, L),
                vmem(n * 8 + 8, 128), vmem(n * 8 + 8, 128), vmem(n * 8 + 8, 128), vmem(n * 8 + 8, 128),
                vmem(256, L), vmem(3, 2, 16, L), vmem(20, 4, 2, 2 * L),
                vmem(2, FIELDS, 24, L), vmem(3, 18, 2, L), vmem(3, 18, 2, L),
                vmem(3, 18, 4, L), vmem(3, 18, 4, L), vmem(3, 20, L), vmem(3, 20, L),
                vmem(2, 80, L), vmem(20, 2, 24, L),
                dma(), dma(),
                dma(10), dma(10), dma(8), dma(8),
                dma(2), dma(2), dma(2), dma(2), dma(2), dma(2),
                dma(), dma(), dma(), dma(),
            ],
            compiler_params=pltpu.CompilerParams(
                collective_id=0, has_side_effects=True, vmem_limit_bytes=16 * 2**20
            ),
        )(density, populations)
        return pl.pallas_call(
            put,
            out_shape=shapes,
            in_specs=[any_spec, any_spec],
            out_specs=(any_spec, any_spec),
            scratch_shapes=[dma(), dma()],
            compiler_params=pltpu.CompilerParams(vmem_limit_bytes=8 * 2**20),
        )(density, populations)

    return jax.shard_map(
        local,
        mesh=mesh,
        in_specs=(P("gx", "gy", None), P(None, "gx", "gy", None)),
        out_specs=(P("gx", "gy", None), P(None, "gx", "gy", None)),
        check_vma=False,
    )
```
